32 devices in a mesh: gx: 4 (over y, x), gy: 2 (over core), row: 4 (over z).
Axes of the slice: x: 2, y: 2, z: 4, core: 2. Of those that a mesh axis runs over, the one named last changes fastest.
Arguments:
- occupancy: int32 [32, 512, 1024], P('row', 'gx', 'gy'), may hold values 0 or 1
- random_draws: bfloat16 [4, 32, 512, 1024], P(None, 'row', 'gx', 'gy'), may hold values from 0 to 1
Outputs:
- coverage: float32 [128, 256], P('gx', 'gy')
- projected: float32 [128, 256], P('gx', 'gy')
The draws below stay inside these ranges and needn't reach their ends.
All inputs are finite; a program needn't handle non-finite values. No bound on the sum of `occupancy` on one device may be relied on, other than what follows from the above.
Results may differ from the reference program's by a relative error of at most 0.0003.
Values may be sent and summed in bfloat16 or wider, within the bound.
No kernel may reach another device: no remote copies, remote signals or barrier semaphores. Data moves between devices by JAX's collectives and lax.ppermute only.
A program may use at most 64 MiB of HBM per device.

```python
import jax
import jax.numpy as jnp
from jax import lax

SWEEPS = 4
BLOCK = 4
LEAP = 8
NX = 512
NY = 1024
REAL = 32


def touch_ends(entries, own_key, smallest, top_value):
    extent = entries.shape
    index_at = [jax.random.randint(jax.random.fold_in(own_key, axis), (), 0, extent[axis]) for axis in range(len(extent))]
    entries = entries.at[tuple(index_at)].set(smallest)
    longest = extent.index(max(extent))
    index_at[longest] = (index_at[longest] + 1) % extent[longest]
    return entries.at[tuple(index_at)].set(top_value)


def levels(own_key, extent, shards, smallest, largest):
    gain, own = 1.0, jax.random.fold_in(own_key, 6)
    for position, blocks in shards:
        draws = jnp.exp(jax.random.uniform(jax.random.fold_in(own, position), (blocks,), jnp.float32, smallest / len(shards), largest / len(shards)))
        gain = gain * jnp.repeat(draws, extent[position] // blocks).reshape([-1 if axis == position else 1 for axis in range(len(extent))])
    return gain


def setup_inputs(seed: int = 0) -> dict:
    key_list = jax.random.split(jax.random.key(seed), 3)
    return {
        "occupancy": touch_ends((jax.random.randint(key_list[0], (REAL, NX, NY), 0, 2) < 1).astype(jnp.int32), jax.random.fold_in(key_list[0], 1), 0, 1),
        "random_draws": jnp.clip(1.0 * jax.random.uniform(key_list[1], (SWEEPS, REAL, NX, NY), jnp.float32) ** levels(key_list[1], (SWEEPS, REAL, NX, NY), ((1, 4), (2, 4), (3, 2)), -0.2, 0.2), 0.0, 1.0).astype(jnp.bfloat16),
    }


ADSORB = 0.6
DESORB = 0.6
HOPPING = 0.3
COUPLING = 0.5


def sublattice_update(padded, jitter, colour):
    centre = padded[..., 1:-1, 1:-1]
    beside = padded[..., 2:, 1:-1] + padded[..., :-2, 1:-1] + padded[..., 1:-1, 2:] + padded[..., 1:-1, :-2]
    updated = centre + ADSORB * jitter * (1.0 - centre) - DESORB * (1.0 - jitter) * jnp.exp(-COUPLING * beside) * centre + HOPPING * (0.25 * beside - centre)
    row_index = lax.broadcasted_iota(jnp.int32, centre.shape[-2:], 0)
    col_index = lax.broadcasted_iota(jnp.int32, centre.shape[-2:], 1)
    chosen = ((row_index + col_index + colour) % 2) == 0
    return jnp.where(chosen, updated, centre)


def block_sums(field):
    height, width = field.shape[-2], field.shape[-1]
    shaped = field.reshape(field.shape[:-2] + (height // BLOCK, BLOCK, width // BLOCK, BLOCK))
    return jnp.sum(shaped, axis=(-3, -1))


def one_realization(index, occupancy, random_draws):
    occupied = occupancy[index].astype(jnp.float32)
    earlier = occupied
    for sweep_index in range(SWEEPS):
        if sweep_index == SWEEPS - 2:
            earlier = occupied
        padded = jnp.pad(occupied, 1, mode="wrap")
        occupied = sublattice_update(padded, random_draws[sweep_index, index].astype(jnp.float32), sweep_index % 2)
    return jnp.stack([block_sums(earlier), block_sums(occupied)])


def reference(occupancy, random_draws):
    def mapped(index):
        return one_realization(index, occupancy, random_draws)
    coarse_each = lax.map(mapped, jnp.arange(REAL, dtype=jnp.int32))
    averages = jnp.sum(coarse_each, axis=0) / jnp.float32(REAL * BLOCK * BLOCK)
    coverage = averages[1]
    projected = coverage + (LEAP / 2.0) * (coverage - averages[0])
    return coverage, projected
```

```python
import functools
import math

import jax
import jax.numpy as jnp
from jax import lax
from jax.experimental import pallas as pl
from jax.experimental.pallas import tpu as pltpu
from jax.sharding import PartitionSpec as P

SWEEPS = 4
BLOCK = 4
LEAP = 8

ADSORB = 0.6
DESORB = 0.6
HOPPING = 0.3
COUPLING = 0.5

LANES = 128
GROUP = 16
F32 = jnp.float32
BF16 = jnp.bfloat16
MIB = 1 << 20


def iota(shape, dim):
    return lax.broadcasted_iota(jnp.int32, shape, dim)


def even_lanes(shape):
    return iota(shape, len(shape) - 1) % 2 == 0


def updated(centre, beside, draw):
    gone = 1.0 - jnp.exp2(beside * (-COUPLING * math.log2(math.e)))
    gain = ADSORB * draw
    keep = (1.0 - HOPPING - ADSORB) + (ADSORB - gain) * gone
    return centre * keep + (gain + (0.25 * HOPPING) * beside)


def fold_lanes(width, first, rows_per=1):
    source = iota((width, LANES), 0)
    target = iota((width, LANES), 1)
    return jnp.where(source // BLOCK + first == target, 1.0, 0.0).astype(F32)


def exact_dot(a, b):
    return jnp.dot(a, b, preferred_element_type=F32, precision=lax.Precision.HIGHEST)


def edges_kernel(occ, draws, low, high, obuf, dbuf, sems):
    reals, height, width = occ.shape
    copies = []
    for side, start in ((0, 0), (1, height - 8)):
        copies.append(
            pltpu.make_async_copy(occ.at[:, pl.ds(start, 8), :], obuf.at[side], sems.at[side, 0])
        )
        copies.append(
            pltpu.make_async_copy(
                draws.at[pl.ds(0, 3), :, pl.ds(start, 8), :], dbuf.at[side], sems.at[side, 1]
            )
        )
    for copy in copies:
        copy.start()
    even = even_lanes((8, LANES))
    row = iota((8, LANES), 0)
    even_row = row % 2 == 0

    def by_colour(x):
        swapped = jnp.where(even_row, pltpu.roll(x, 7, 0), pltpu.roll(x, 1, 0))
        return jnp.where(even, x, swapped)

    for side, out in ((0, low), (1, high)):
        copies[2 * side].wait()
        copies[2 * side + 1].wait()
        for r in range(reals):
            for c in range(width // LANES):
                lanes = slice(c * LANES, (c + 1) * LANES)
                first = by_colour(obuf[side, r, :, lanes].astype(F32))
                d0, d1, d2 = (
                    by_colour(dbuf[side, w, r, :, lanes].astype(F32)) for w in range(3)
                )
                mixed = pltpu.roll(jnp.where(even_row, d0, d1), 4, 0)
                if side == 0:
                    message = jnp.where(row < 4, first, jnp.where(row == 7, pltpu.roll(d2, 7, 0), mixed))
                else:
                    message = jnp.where(row >= 4, first, jnp.where(row == 1, pltpu.roll(d2, 3, 0), mixed))
                out[r, c] = message.astype(BF16)


def halo_rows(below, above, name):
    row = iota(below.shape, 0)
    moves = {
        "p0": ((2, 1), (0, 7)),
        "p1": ((1, 0), (7, 6)),
        "u0": ((6, 5), (4, 3)),
        "u1": ((4, 4), (3, 3)),
        "u2": ((6, 6), (1, 1)),
    }[name]
    (a6, a7), (b0, b1) = moves

    def moved(x, by):
        return x if by == 0 else pltpu.roll(x, by, 0)

    top = moved(above, a7) if a6 == a7 else jnp.where(row == 6, moved(above, a6), moved(above, a7))
    low = moved(below, b0) if b0 == b1 else jnp.where(row == 0, moved(below, b0), moved(below, b1))
    return top, low


NAMES = ("p0", "p1", "u0", "u1", "u2")


def tile_kernel(occ, draws, frames, strips, part, obuf, dbuf, natural, state, sums, sems):
    reals, height, width = occ.shape
    pairs = height // 2
    tiles = width // LANES
    sweeps = draws.shape[0]

    def copies(r):
        out = [
            pltpu.make_async_copy(
                occ.at[r, :, pl.ds(c * LANES, LANES)], obuf.at[r, c], sems.at[r, c]
            )
            for c in range(tiles)
        ]
        out.append(pltpu.make_async_copy(draws.at[:, r], dbuf.at[r], sems.at[r, tiles]))
        return out

    @pl.loop(0, reals)
    def _(r):
        for copy in copies(r):
            copy.start()

    even = even_lanes((pairs, LANES))
    lane = iota((pairs, LANES), 1)
    sums[...] = jnp.zeros_like(sums)
    strips[...] = jnp.zeros_like(strips)
    for colour in range(2):
        for c in range(tiles):
            state[colour, c, 0:8] = jnp.zeros((8, LANES), F32)
            state[colour, c, pairs + 8 : pairs + 16] = jnp.zeros((8, LANES), F32)

    @pl.loop(0, reals)
    def _(r):
        for copy in copies(r):
            copy.wait()
        group = lane // GROUP == r
        from_left = group & (lane % GROUP >= BLOCK)

        def keep_edges(index, c, value):
            frames[index, r, 0, c] = value[0:8]
            frames[index, r, 1, c] = value[pairs - 8 : pairs]
            if c == 0:
                strips[index, 0] = jnp.where(
                    from_left, pltpu.roll(value, r * GROUP + BLOCK, 1), strips[index, 0]
                )
            if c == tiles - 1:
                strips[index, 1] = jnp.where(
                    group, pltpu.roll(value, r * GROUP + 12, 1), strips[index, 1]
                )

        for c in range(tiles):
            first = obuf[r, c, pl.ds(0, pairs, stride=2)].astype(F32)
            second = obuf[r, c, pl.ds(1, pairs, stride=2)].astype(F32)
            p0 = jnp.where(even, first, second)
            p1 = jnp.where(even, second, first)
            state[0, c, 8 : 8 + pairs] = p0
            state[1, c, 8 : 8 + pairs] = p1
            keep_edges(0, c, p0)
            keep_edges(1, c, p1)
        for w in range(sweeps):
            colour = w % 2
            for c in range(tiles):
                natural[w, c] = dbuf[r, w, :, c * LANES : (c + 1) * LANES].astype(F32)
            for c in range(tiles):
                first = natural[w, c, pl.ds(0, pairs, stride=2)]
                second = natural[w, c, pl.ds(1, pairs, stride=2)]
                draw = jnp.where(even, first, second) if colour == 0 else jnp.where(even, second, first)
                keep_edges(2 + w, c, draw)
                other = 1 - colour
                here = state[other, c, 8 : 8 + pairs]
                up = state[other, c, 7 : 7 + pairs]
                down = state[other, c, 9 : 9 + pairs]
                vertical = jnp.where(even, up, down) if colour == 0 else jnp.where(even, down, up)
                left = state[other, (c - 1) % tiles, 8 : 8 + pairs]
                right = state[other, (c + 1) % tiles, 8 : 8 + pairs]
                left = pltpu.roll(jnp.where(lane == LANES - 1, left, here), 1, 1)
                right = pltpu.roll(jnp.where(lane == 0, right, here), LANES - 1, 1)
                new = updated(
                    state[colour, c, 8 : 8 + pairs], (here + vertical) + (left + right), draw
                )
                state[colour, c, 8 : 8 + pairs] = new
                if w == sweeps - 3 or w == sweeps - 1:
                    snapshot = 0 if w == sweeps - 3 else 1
                    sums[snapshot, c] += here + new

    half = pairs // 2
    total = jnp.zeros((2 * half, LANES), F32)
    for c in range(tiles):
        rows = jnp.concatenate(
            [
                sums[s, c, pl.ds(0, half, stride=2)] + sums[s, c, pl.ds(1, half, stride=2)]
                for s in range(2)
            ]
        )
        total += exact_dot(rows, fold_lanes(LANES, c * (LANES // BLOCK)))
    part[0] = total[:half]
    part[1] = total[half:]


def strips_kernel(below, above, strips, message, corners):
    reals, tiles = below.shape[:2]
    pairs = strips.shape[2]
    lane = iota((8, LANES), 1)
    for v, source in ((0, above), (1, below)):
        sides = [jnp.zeros((8, LANES), F32) for _ in range(2)]
        for r in range(reals):
            group = lane // GROUP == r
            left = pltpu.roll(source[r, 0].astype(F32), r * GROUP + BLOCK, 1)
            right = pltpu.roll(source[r, tiles - 1].astype(F32), (r * GROUP + 12) % LANES, 1)
            sides[0] = jnp.where(group & (lane % GROUP >= BLOCK), left, sides[0])
            sides[1] = jnp.where(group, right, sides[1])
        corners[0, v] = sides[0]
        corners[1, v] = sides[1]
        message[len(NAMES) * pairs + 8 * v : len(NAMES) * pairs + 8 * v + 8] = jnp.where(
            lane % GROUP < 8, sides[0], sides[1]
        ).astype(BF16)
    lane = iota((pairs, LANES), 1)
    for index in range(len(NAMES)):
        message[index * pairs : (index + 1) * pairs] = jnp.where(
            lane % GROUP < 8, strips[index, 0], strips[index, 1]
        ).astype(BF16)


def rows_kernel(below, above, frames, out, arrays):
    reals, tiles = below.shape[:2]
    sweeps = frames.shape[0] - 2
    even = even_lanes((8, LANES))
    lane = iota((8, LANES), 1)
    row = iota((8, LANES), 0)
    sides = range(2)
    for r in range(reals):
        for c in range(tiles):
            low = below[r, c].astype(F32)
            high = above[r, c].astype(F32)
            for index, name in enumerate(NAMES):
                top, bottom = halo_rows(low, high, name)
                arrays[index, r, 0, c] = jnp.where(row >= 6, top, frames[index, r, 0, c])
                arrays[index, r, 1, c] = jnp.where(row < 2, bottom, frames[index, r, 1, c])
    sums = [[[None] * tiles for _ in sides] for _ in range(2)]
    for w in range(sweeps):
        colour = w % 2
        other = 1 - colour
        for r in range(reals):
            for side in sides:
                for c in range(tiles):
                    draw = arrays[2 + w, r, side, c] if w < 3 else frames[2 + w, r, side, c]
                    here = arrays[other, r, side, c]
                    up = pltpu.roll(here, 1, 0)
                    down = pltpu.roll(here, 7, 0)
                    vertical = jnp.where(even, up, down) if colour == 0 else jnp.where(even, down, up)
                    left = arrays[other, r, side, (c - 1) % tiles]
                    right = arrays[other, r, side, (c + 1) % tiles]
                    left = pltpu.roll(jnp.where(lane == LANES - 1, left, here), 1, 1)
                    right = pltpu.roll(jnp.where(lane == 0, right, here), LANES - 1, 1)
                    new = updated(
                        arrays[colour, r, side, c], (here + vertical) + (left + right), draw
                    )
                    arrays[colour, r, side, c] = new
                    if w == sweeps - 3 or w == sweeps - 1:
                        s = 0 if w == sweeps - 3 else 1
                        both = here + new
                        before = sums[s][side][c]
                        sums[s][side][c] = both if before is None else before + both
    total = jnp.zeros((8, LANES), F32)
    for c in range(tiles):
        rows = jnp.zeros((8, LANES), F32)
        for s in range(2):
            for side in sides:
                both = sums[s][side][c]
                both = both + pltpu.roll(both, 1, 0)
                index = 2 * s + side
                shift = (index - (1 if side == 0 else 7)) % 8
                both = both if shift == 0 else pltpu.roll(both, shift, 0)
                rows = jnp.where(row == index, both, rows)
        total += exact_dot(rows, fold_lanes(LANES, c * (LANES // BLOCK)))
    out[...] = total


def columns_kernel(strips, corners, from_left, from_right, part, rows, out, arrays):
    pairs = strips.shape[2]
    sweeps = strips.shape[0] - 2
    base = 16
    count = len(NAMES)
    lane = iota((pairs, LANES), 1) % GROUP
    lane8 = iota((8, LANES), 1) % GROUP
    row8 = iota((8, LANES), 0)

    def joined(side, q, own, left, right):
        if side == 0:
            return jnp.where(q < BLOCK, pltpu.roll(left, LANES - 8, 1), own)
        return jnp.where(q >= GROUP - BLOCK, pltpu.roll(right, 8, 1), own)

    zero = jnp.zeros((8, LANES), F32)
    for side in range(2):
        for index in range(count):
            rows_of = slice(index * pairs, (index + 1) * pairs)
            arrays[index, side, base : base + pairs] = joined(
                side, lane, strips[index, side], from_left[rows_of].astype(F32), from_right[rows_of].astype(F32)
            )
        halos = []
        for v in range(2):
            rows_of = slice(count * pairs + 8 * v, count * pairs + 8 * v + 8)
            halos.append(
                joined(side, lane8, corners[side, v], from_left[rows_of].astype(F32), from_right[rows_of].astype(F32))
            )
        for index, name in enumerate(NAMES):
            top, bottom = halo_rows(halos[1], halos[0], name)
            arrays[index, side, base - 8 : base] = jnp.where(row8 >= 6, top, 0.0)
            arrays[index, side, base + pairs : base + pairs + 8] = jnp.where(row8 < 2, bottom, 0.0)
            if index < 2:
                arrays[index, side, 0 : base - 8] = zero
                arrays[index, side, base + pairs + 8 : base + pairs + 16] = zero
        arrays[count, side, base : base + pairs] = strips[count, side]
        arrays[count, side, base - 8 : base] = zero
        arrays[count, side, base + pairs : base + pairs + 8] = zero
    half = pairs // 2
    sums = [[None, None], [None, None]]
    for w in range(sweeps):
        colour = w % 2
        other = 1 - colour
        grow = 8 if w < sweeps - 1 else 0
        start, size = base - grow, pairs + 2 * grow
        even = even_lanes((size, LANES))
        for side in range(2):
            here = arrays[other, side, start : start + size]
            up = arrays[other, side, start - 1 : start - 1 + size]
            down = arrays[other, side, start + 1 : start + 1 + size]
            vertical = jnp.where(even, up, down) if colour == 0 else jnp.where(even, down, up)
            beside = (here + vertical) + (pltpu.roll(here, 1, 1) + pltpu.roll(here, LANES - 1, 1))
            new = updated(
                arrays[colour, side, start : start + size], beside, arrays[2 + w, side, start : start + size]
            )
            arrays[colour, side, start : start + size] = new
            if w == sweeps - 3 or w == sweeps - 1:
                s = 0 if w == sweeps - 3 else 1
                arrays[count + 1 + s, side, base : base + pairs] = (here + new)[grow : grow + pairs]
    source = iota((LANES, LANES), 0) % GROUP
    target = iota((LANES, LANES), 1)
    total = jnp.zeros((2 * half, LANES), F32)
    for side in range(2):
        rows_of = jnp.concatenate(
            [
                arrays[count + 1 + s, side, pl.ds(base, half, stride=2)]
                + arrays[count + 1 + s, side, pl.ds(base + 1, half, stride=2)]
                for s in range(2)
            ]
        )
        first = BLOCK if side == 0 else 2 * BLOCK
        pick = (source >= first) & (source < first + BLOCK) & (target == (0 if side == 0 else LANES - 1))
        total += exact_dot(rows_of, jnp.where(pick, 1.0, 0.0).astype(F32))
    row = iota((half, LANES), 0)
    column = iota((half, LANES), 1)
    for s in range(2):
        value = part[s]
        value = jnp.where(row == 0, rows[2 * s : 2 * s + 1], value)
        value = jnp.where(row == half - 1, rows[2 * s + 1 : 2 * s + 2], value)
        edge = (column == 0) | (column == LANES - 1)
        out[s] = jnp.where(edge, total[s * half : (s + 1) * half], value)


def shifted(value, axis, by):
    count = lax.axis_size(axis)
    if count == 1:
        return value
    return lax.ppermute(value, axis, [(i, (i + by) % count) for i in range(count)])


def both_ways(to_low, to_high, axis):
    return shifted(to_low, axis, -1), shifted(to_high, axis, 1)


def call(kernel, args, outs, name, vmem, scratch=(), flops=0, space=pltpu.VMEM):
    return pl.pallas_call(
        kernel,
        out_shape=tuple(pltpu.VMEM(shape, dtype) for shape, dtype in outs),
        in_specs=[pl.BlockSpec(memory_space=space) for _ in args],
        out_specs=tuple(pl.BlockSpec(memory_space=pltpu.VMEM) for _ in outs),
        scratch_shapes=list(scratch),
        name=name,
        compiler_params=pltpu.CompilerParams(vmem_limit_bytes=vmem * MIB),
        cost_estimate=pl.CostEstimate(flops=flops, bytes_accessed=0, transcendentals=0),
    )(*args)


def per_device(occupancy, random_draws):
    reals, height, width = occupancy.shape
    sweeps = random_draws.shape[0]
    tiles, pairs, half = width // LANES, height // 2, height // BLOCK
    edge = ((reals, tiles, 8, LANES), BF16)
    low, high = call(
        edges_kernel,
        (occupancy, random_draws),
        (edge, edge),
        "edges",
        8,
        (
            pltpu.VMEM((2, reals, 8, width), jnp.int32),
            pltpu.VMEM((2, 3, reals, 8, width), BF16),
            pltpu.SemaphoreType.DMA((2, 2)),
        ),
        1_000_000,
        pl.ANY,
    )
    below, above = both_ways(low, high, "gx")
    frames, strips, part = call(
        tile_kernel,
        (occupancy, random_draws),
        (
            ((2 + sweeps, reals, 2, tiles, 8, LANES), F32),
            ((2 + sweeps, 2, pairs, LANES), F32),
            ((2, half, LANES), F32),
        ),
        "tile",
        24,
        (
            pltpu.VMEM((reals, tiles, height, LANES), jnp.int32),
            pltpu.VMEM((reals, sweeps, height, width), BF16),
            pltpu.VMEM((sweeps, tiles, height, LANES), F32),
            pltpu.VMEM((2, tiles, pairs + 16, LANES), F32),
            pltpu.VMEM((2, tiles, pairs, LANES), F32),
            pltpu.SemaphoreType.DMA((reals, tiles + 1)),
        ),
        40_000_000,
        pl.ANY,
    )
    message, corners = call(
        strips_kernel,
        (below, above, strips),
        (((len(NAMES) * pairs + 16, LANES), BF16), ((2, 2, 8, LANES), F32)),
        "strips",
        4,
        (),
        1_000_000,
    )
    if lax.axis_size("gy") == 2:
        from_left = from_right = shifted(message, "gy", 1)
    else:
        from_right, from_left = both_ways(message, message, "gy")
    (rows,) = call(
        rows_kernel,
        (below, above, frames),
        (((8, LANES), F32),),
        "rows",
        8,
        (pltpu.VMEM((len(NAMES), reals, 2, tiles, 8, LANES), F32),),
        10_000_000,
    )
    (mine,) = call(
        columns_kernel,
        (strips, corners, from_left, from_right, part, rows),
        (((2, half, LANES), F32),),
        "columns",
        8,
        (pltpu.VMEM((len(NAMES) + 3, 2, pairs + 32, LANES), F32),),
        4_000_000,
    )
    count = lax.axis_size("row")
    if count == 4:
        one, two, three = (shifted(mine, "row", by) for by in (1, 2, 3))
        coarse_sums = (mine + two) + (one + three)
    else:
        coarse_sums = lax.psum(mine, "row")
    averages = coarse_sums * jnp.float32(1.0 / (reals * count * BLOCK * BLOCK))
    coverage = averages[1]
    projected = coverage + LEAP / 2.0 * (coverage - averages[0])
    return (coverage, projected)


def solution(mesh):
    in_specs = (P("row", "gx", "gy"), P(None, "row", "gx", "gy"))
    out_specs = (P("gx", "gy"), P("gx", "gy"))
    return jax.shard_map(
        per_device, mesh=mesh, in_specs=in_specs, out_specs=out_specs, check_vma=False
    )
```

```python
import functools
import math

import jax
import jax.numpy as jnp
from jax import lax
from jax.experimental import pallas as pl
from jax.experimental.pallas import tpu as pltpu
from jax.sharding import PartitionSpec as P

SWEEPS = 4
BLOCK = 4
LEAP = 8

ADSORB = 0.6
DESORB = 0.6
HOPPING = 0.3
COUPLING = 0.5

LANES = 128
CHUNK = 8
GROUP = 16
F32 = jnp.float32
BF16 = jnp.bfloat16
MIB = 1 << 20


def iota(shape, dim):
    return lax.broadcasted_iota(jnp.int32, shape, dim)


def even_lanes(shape):
    return iota(shape, len(shape) - 1) % 2 == 0


def updated(centre, beside, draw):
    gone = 1.0 - jnp.exp2(beside * (-COUPLING * math.log2(math.e)))
    gain = ADSORB * draw
    keep = (1.0 - HOPPING - ADSORB) + (ADSORB - gain) * gone
    return centre * keep + (gain + (0.25 * HOPPING) * beside)


def fold_lanes(first):
    source = iota((LANES, LANES), 0)
    target = iota((LANES, LANES), 1)
    return selection(source // BLOCK + first == target)


def selection(picked):
    return jnp.where(picked, 1.0, 0.0).astype(BF16)


def split(x):
    high = x.astype(BF16)
    rest = x - high.astype(F32)
    middle = rest.astype(BF16)
    low = (rest - middle.astype(F32)).astype(BF16)
    return jnp.concatenate([high, middle, low])


def selected(x, matrix):
    size = x.shape[0]
    y = jnp.dot(split(x), matrix, preferred_element_type=F32)
    return (y[:size] + y[size : 2 * size]) + y[2 * size :]


def edges_kernel(occ, draws, low, high, obuf, dbuf, sems):
    reals, height, width = occ.shape
    copies = []
    for side, start in ((0, 0), (1, height - 8)):
        copies.append(
            pltpu.make_async_copy(occ.at[:, pl.ds(start, 8), :], obuf.at[side], sems.at[side, 0])
        )
        copies.append(
            pltpu.make_async_copy(
                draws.at[pl.ds(0, 3), :, pl.ds(start, 8), :], dbuf.at[side], sems.at[side, 1]
            )
        )
    for copy in copies:
        copy.start()
    even = even_lanes((8, LANES))
    row = iota((8, LANES), 0)
    even_row = row % 2 == 0

    def by_colour(x):
        swapped = jnp.where(even_row, pltpu.roll(x, 7, 0), pltpu.roll(x, 1, 0))
        return jnp.where(even, x, swapped)

    for side, out in ((0, low), (1, high)):
        copies[2 * side].wait()
        copies[2 * side + 1].wait()
        for r in range(reals):
            for c in range(width // LANES):
                lanes = slice(c * LANES, (c + 1) * LANES)
                first = by_colour(obuf[side, r, :, lanes].astype(F32))
                d0, d1, d2 = (
                    by_colour(dbuf[side, w, r, :, lanes].astype(F32)) for w in range(3)
                )
                mixed = pltpu.roll(jnp.where(even_row, d0, d1), 4, 0)
                if side == 0:
                    message = jnp.where(row < 4, first, jnp.where(row == 7, pltpu.roll(d2, 7, 0), mixed))
                else:
                    message = jnp.where(row >= 4, first, jnp.where(row == 1, pltpu.roll(d2, 3, 0), mixed))
                out[r, c] = message.astype(BF16)


def halo_rows(below, above, name):
    row = iota(below.shape, 0)
    moves = {
        "p0": ((2, 1), (0, 7)),
        "p1": ((1, 0), (7, 6)),
        "u0": ((6, 5), (4, 3)),
        "u1": ((4, 4), (3, 3)),
        "u2": ((6, 6), (1, 1)),
    }[name]
    (a6, a7), (b0, b1) = moves

    def moved(x, by):
        return x if by == 0 else pltpu.roll(x, by, 0)

    top = moved(above, a7) if a6 == a7 else jnp.where(row == 6, moved(above, a6), moved(above, a7))
    low = moved(below, b0) if b0 == b1 else jnp.where(row == 0, moved(below, b0), moved(below, b1))
    return top, low


NAMES = ("p0", "p1", "u0", "u1", "u2")


def tile_kernel(occ, draws, frames, strips, part, obuf, dbuf, natural, state, sums, sems):
    reals, height, width = occ.shape
    pairs = height // 2
    tiles = width // LANES
    sweeps = draws.shape[0]

    def copies(r):
        out = [
            pltpu.make_async_copy(
                occ.at[r, :, pl.ds(c * LANES, LANES)], obuf.at[r, c], sems.at[r, c]
            )
            for c in range(tiles)
        ]
        out.append(pltpu.make_async_copy(draws.at[:, r], dbuf.at[r], sems.at[r, tiles]))
        return out

    @pl.loop(0, reals)
    def _(r):
        for copy in copies(r):
            copy.start()

    even = even_lanes((CHUNK, LANES))
    lane = iota((CHUNK, LANES), 1)
    sums[...] = jnp.zeros_like(sums)
    strips[...] = jnp.zeros_like(strips)
    for colour in range(2):
        for c in range(tiles):
            state[colour, c, 0:8] = jnp.zeros((8, LANES), F32)
            state[colour, c, pairs + 8 : pairs + 16] = jnp.zeros((8, LANES), F32)

    @pl.loop(0, reals)
    def _(r):
        for copy in copies(r):
            copy.wait()
        group = lane // GROUP == r
        from_left = group & (lane % GROUP >= BLOCK)

        def keep_edges(index, c, value, start):
            if start == 0:
                frames[index, r, 0, c] = value[:8]
            if start == pairs - CHUNK:
                frames[index, r, 1, c] = value[CHUNK - 8 :]
            rows = slice(start, start + CHUNK)
            if c == 0:
                pltpu.store(strips.at[index, 0, rows], pltpu.roll(value, r * GROUP + BLOCK, 1), mask=from_left)
            if c == tiles - 1:
                pltpu.store(strips.at[index, 1, rows], pltpu.roll(value, r * GROUP + 12, 1), mask=group)

        for start in range(0, pairs, CHUNK):
            for c in range(tiles):
                first = obuf[r, c, pl.ds(2 * start, CHUNK, stride=2)].astype(F32)
                second = obuf[r, c, pl.ds(2 * start + 1, CHUNK, stride=2)].astype(F32)
                p0 = jnp.where(even, first, second)
                p1 = jnp.where(even, second, first)
                state[0, c, 8 + start : 8 + start + CHUNK] = p0
                state[1, c, 8 + start : 8 + start + CHUNK] = p1
                keep_edges(0, c, p0, start)
                keep_edges(1, c, p1, start)
        for w in range(sweeps):
            colour = w % 2
            other = 1 - colour
            for c in range(tiles):
                natural[w, c] = dbuf[r, w, :, c * LANES : (c + 1) * LANES].astype(F32)
            for start in range(0, pairs, CHUNK):
                heres = [state[other, c, 8 + start : 8 + start + CHUNK] for c in range(tiles)]
                for c in range(tiles):
                    first = natural[w, c, pl.ds(2 * start, CHUNK, stride=2)]
                    second = natural[w, c, pl.ds(2 * start + 1, CHUNK, stride=2)]
                    draw = jnp.where(even, first, second) if colour == 0 else jnp.where(even, second, first)
                    keep_edges(2 + w, c, draw, start)
                    here = heres[c]
                    up = state[other, c, 7 + start : 7 + start + CHUNK]
                    down = state[other, c, 9 + start : 9 + start + CHUNK]
                    vertical = jnp.where(even, up, down) if colour == 0 else jnp.where(even, down, up)
                    left = jnp.where(lane == LANES - 1, heres[(c - 1) % tiles], here)
                    right = jnp.where(lane == 0, heres[(c + 1) % tiles], here)
                    beside = pltpu.roll(left, 1, 1) + pltpu.roll(right, LANES - 1, 1)
                    new = updated(
                        state[colour, c, 8 + start : 8 + start + CHUNK], (here + vertical) + beside, draw
                    )
                    state[colour, c, 8 + start : 8 + start + CHUNK] = new
                    if w == sweeps - 3 or w == sweeps - 1:
                        snapshot = 0 if w == sweeps - 3 else 1
                        sums[snapshot, c, start : start + CHUNK] += here + new

    half = pairs // 2
    total = jnp.zeros((2 * half, LANES), F32)
    for c in range(tiles):
        rows = jnp.concatenate(
            [
                sums[s, c, pl.ds(0, half, stride=2)] + sums[s, c, pl.ds(1, half, stride=2)]
                for s in range(2)
            ]
        )
        total += selected(rows, fold_lanes(c * (LANES // BLOCK)))
    part[0] = total[:half]
    part[1] = total[half:]


def strips_kernel(below, above, strips, message, corners):
    reals, tiles = below.shape[:2]
    pairs = strips.shape[2]
    lane = iota((8, LANES), 1)
    for v, source in ((0, above), (1, below)):
        sides = [jnp.zeros((8, LANES), F32) for _ in range(2)]
        for r in range(reals):
            group = lane // GROUP == r
            left = pltpu.roll(source[r, 0].astype(F32), r * GROUP + BLOCK, 1)
            right = pltpu.roll(source[r, tiles - 1].astype(F32), (r * GROUP + 12) % LANES, 1)
            sides[0] = jnp.where(group & (lane % GROUP >= BLOCK), left, sides[0])
            sides[1] = jnp.where(group, right, sides[1])
        corners[0, v] = sides[0]
        corners[1, v] = sides[1]
        message[len(NAMES) * pairs + 8 * v : len(NAMES) * pairs + 8 * v + 8] = jnp.where(
            lane % GROUP < 8, sides[0], sides[1]
        ).astype(BF16)
    lane = iota((pairs, LANES), 1)
    for index in range(len(NAMES)):
        message[index * pairs : (index + 1) * pairs] = jnp.where(
            lane % GROUP < 8, strips[index, 0], strips[index, 1]
        ).astype(BF16)


def rows_kernel(below, above, frames, out, arrays):
    reals, tiles = below.shape[:2]
    sweeps = frames.shape[0] - 2
    even = even_lanes((8, LANES))
    lane = iota((8, LANES), 1)
    row = iota((8, LANES), 0)
    sides = range(2)
    for r in range(reals):
        for c in range(tiles):
            low = below[r, c].astype(F32)
            high = above[r, c].astype(F32)
            for index, name in enumerate(NAMES):
                top, bottom = halo_rows(low, high, name)
                arrays[index, r, 0, c] = jnp.where(row >= 6, top, frames[index, r, 0, c])
                arrays[index, r, 1, c] = jnp.where(row < 2, bottom, frames[index, r, 1, c])
    sums = [[[None] * tiles for _ in sides] for _ in range(2)]
    for w in range(sweeps):
        colour = w % 2
        other = 1 - colour
        for r in range(reals):
            for side in sides:
                for c in range(tiles):
                    draw = arrays[2 + w, r, side, c] if w < 3 else frames[2 + w, r, side, c]
                    here = arrays[other, r, side, c]
                    up = pltpu.roll(here, 1, 0)
                    down = pltpu.roll(here, 7, 0)
                    vertical = jnp.where(even, up, down) if colour == 0 else jnp.where(even, down, up)
                    left = arrays[other, r, side, (c - 1) % tiles]
                    right = arrays[other, r, side, (c + 1) % tiles]
                    left = pltpu.roll(jnp.where(lane == LANES - 1, left, here), 1, 1)
                    right = pltpu.roll(jnp.where(lane == 0, right, here), LANES - 1, 1)
                    new = updated(
                        arrays[colour, r, side, c], (here + vertical) + (left + right), draw
                    )
                    arrays[colour, r, side, c] = new
                    if w == sweeps - 3 or w == sweeps - 1:
                        s = 0 if w == sweeps - 3 else 1
                        both = here + new
                        before = sums[s][side][c]
                        sums[s][side][c] = both if before is None else before + both
    total = jnp.zeros((8, LANES), F32)
    for c in range(tiles):
        rows = jnp.zeros((8, LANES), F32)
        for s in range(2):
            for side in sides:
                both = sums[s][side][c]
                both = both + pltpu.roll(both, 1, 0)
                index = 2 * s + side
                shift = (index - (1 if side == 0 else 7)) % 8
                both = both if shift == 0 else pltpu.roll(both, shift, 0)
                rows = jnp.where(row == index, both, rows)
        total += selected(rows, fold_lanes(c * (LANES // BLOCK)))
    out[...] = total


def columns_kernel(strips, corners, from_left, from_right, part, rows, out, arrays):
    pairs = strips.shape[2]
    sweeps = strips.shape[0] - 2
    base = 16
    count = len(NAMES)
    lane = iota((pairs, LANES), 1) % GROUP
    lane8 = iota((8, LANES), 1) % GROUP
    row8 = iota((8, LANES), 0)

    def joined(side, q, own, left, right):
        if side == 0:
            return jnp.where(q < BLOCK, pltpu.roll(left, LANES - 8, 1), own)
        return jnp.where(q >= GROUP - BLOCK, pltpu.roll(right, 8, 1), own)

    zero = jnp.zeros((8, LANES), F32)
    for side in range(2):
        for index in range(count):
            rows_of = slice(index * pairs, (index + 1) * pairs)
            arrays[index, side, base : base + pairs] = joined(
                side, lane, strips[index, side], from_left[rows_of].astype(F32), from_right[rows_of].astype(F32)
            )
        halos = []
        for v in range(2):
            rows_of = slice(count * pairs + 8 * v, count * pairs + 8 * v + 8)
            halos.append(
                joined(side, lane8, corners[side, v], from_left[rows_of].astype(F32), from_right[rows_of].astype(F32))
            )
        for index, name in enumerate(NAMES):
            top, bottom = halo_rows(halos[1], halos[0], name)
            arrays[index, side, base - 8 : base] = jnp.where(row8 >= 6, top, 0.0)
            arrays[index, side, base + pairs : base + pairs + 8] = jnp.where(row8 < 2, bottom, 0.0)
            if index < 2:
                arrays[index, side, 0 : base - 8] = zero
                arrays[index, side, base + pairs + 8 : base + pairs + 16] = zero
        arrays[count, side, base : base + pairs] = strips[count, side]
        arrays[count, side, base - 8 : base] = zero
        arrays[count, side, base + pairs : base + pairs + 8] = zero
    half = pairs // 2
    sums = [[None, None], [None, None]]
    for w in range(sweeps):
        colour = w % 2
        other = 1 - colour
        grow = 8 if w < sweeps - 1 else 0
        start, size = base - grow, pairs + 2 * grow
        even = even_lanes((size, LANES))
        for side in range(2):
            here = arrays[other, side, start : start + size]
            up = arrays[other, side, start - 1 : start - 1 + size]
            down = arrays[other, side, start + 1 : start + 1 + size]
            vertical = jnp.where(even, up, down) if colour == 0 else jnp.where(even, down, up)
            beside = (here + vertical) + (pltpu.roll(here, 1, 1) + pltpu.roll(here, LANES - 1, 1))
            new = updated(
                arrays[colour, side, start : start + size], beside, arrays[2 + w, side, start : start + size]
            )
            arrays[colour, side, start : start + size] = new
            if w == sweeps - 3 or w == sweeps - 1:
                s = 0 if w == sweeps - 3 else 1
                arrays[count + 1 + s, side, base : base + pairs] = (here + new)[grow : grow + pairs]
    source = iota((LANES, LANES), 0) % GROUP
    target = iota((LANES, LANES), 1)
    total = jnp.zeros((2 * half, LANES), F32)
    for side in range(2):
        rows_of = jnp.concatenate(
            [
                arrays[count + 1 + s, side, pl.ds(base, half, stride=2)]
                + arrays[count + 1 + s, side, pl.ds(base + 1, half, stride=2)]
                for s in range(2)
            ]
        )
        first = BLOCK if side == 0 else 2 * BLOCK
        pick = (source >= first) & (source < first + BLOCK) & (target == (0 if side == 0 else LANES - 1))
        total += selected(rows_of, selection(pick))
    row = iota((half, LANES), 0)
    column = iota((half, LANES), 1)
    for s in range(2):
        value = part[s]
        value = jnp.where(row == 0, rows[2 * s : 2 * s + 1], value)
        value = jnp.where(row == half - 1, rows[2 * s + 1 : 2 * s + 2], value)
        edge = (column == 0) | (column == LANES - 1)
        out[s] = jnp.where(edge, total[s * half : (s + 1) * half], value)


def shifted(value, axis, by):
    count = lax.axis_size(axis)
    if count == 1:
        return value
    return lax.ppermute(value, axis, [(i, (i + by) % count) for i in range(count)])


def both_ways(to_low, to_high, axis):
    return shifted(to_low, axis, -1), shifted(to_high, axis, 1)


def call(kernel, args, outs, name, vmem, scratch=(), flops=0, space=pltpu.VMEM):
    if space == pltpu.HBM:
        args = [pltpu.with_memory_space_constraint(arg, space) for arg in args]
    return pl.pallas_call(
        kernel,
        out_shape=tuple(pltpu.VMEM(shape, dtype) for shape, dtype in outs),
        in_specs=[pl.BlockSpec(memory_space=space) for _ in args],
        out_specs=tuple(pl.BlockSpec(memory_space=pltpu.VMEM) for _ in outs),
        scratch_shapes=list(scratch),
        name=name,
        compiler_params=pltpu.CompilerParams(vmem_limit_bytes=vmem * MIB),
        cost_estimate=pl.CostEstimate(flops=flops, bytes_accessed=0, transcendentals=0),
    )(*args)


def per_device(occupancy, random_draws):
    reals, height, width = occupancy.shape
    sweeps = random_draws.shape[0]
    tiles, pairs, half = width // LANES, height // 2, height // BLOCK
    edge = ((reals, tiles, 8, LANES), BF16)
    low, high = call(
        edges_kernel,
        (occupancy, random_draws),
        (edge, edge),
        "edges",
        8,
        (
            pltpu.VMEM((2, reals, 8, width), jnp.int32),
            pltpu.VMEM((2, 3, reals, 8, width), BF16),
            pltpu.SemaphoreType.DMA((2, 2)),
        ),
        1_000_000,
        pltpu.HBM,
    )
    below, above = both_ways(low, high, "gx")
    frames, strips, part = call(
        tile_kernel,
        (occupancy, random_draws),
        (
            ((2 + sweeps, reals, 2, tiles, 8, LANES), F32),
            ((2 + sweeps, 2, pairs, LANES), F32),
            ((2, half, LANES), F32),
        ),
        "tile",
        24,
        (
            pltpu.VMEM((reals, tiles, height, LANES), jnp.int32),
            pltpu.VMEM((reals, sweeps, height, width), BF16),
            pltpu.VMEM((sweeps, tiles, height, LANES), F32),
            pltpu.VMEM((2, tiles, pairs + 16, LANES), F32),
            pltpu.VMEM((2, tiles, pairs, LANES), F32),
            pltpu.SemaphoreType.DMA((reals, tiles + 1)),
        ),
        40_000_000,
        pltpu.HBM,
    )
    message, corners = call(
        strips_kernel,
        (below, above, strips),
        (((len(NAMES) * pairs + 16, LANES), BF16), ((2, 2, 8, LANES), F32)),
        "strips",
        4,
        (),
        1_000_000,
    )
    if lax.axis_size("gy") == 2:
        from_left = from_right = shifted(message, "gy", 1)
    else:
        from_right, from_left = both_ways(message, message, "gy")
    (rows,) = call(
        rows_kernel,
        (below, above, frames),
        (((8, LANES), F32),),
        "rows",
        8,
        (pltpu.VMEM((len(NAMES), reals, 2, tiles, 8, LANES), F32),),
        10_000_000,
    )
    (mine,) = call(
        columns_kernel,
        (strips, corners, from_left, from_right, part, rows),
        (((2, half, LANES), F32),),
        "columns",
        8,
        (pltpu.VMEM((len(NAMES) + 3, 2, pairs + 32, LANES), F32),),
        4_000_000,
    )
    count = lax.axis_size("row")
    if count == 4:
        one, three, two = (shifted(mine, "row", by) for by in (1, 3, 2))
        coarse_sums = (mine + two) + (one + three)
    else:
        coarse_sums = lax.psum(mine, "row")
    averages = coarse_sums * jnp.float32(1.0 / (reals * count * BLOCK * BLOCK))
    coverage = averages[1]
    projected = coverage + LEAP / 2.0 * (coverage - averages[0])
    return (coverage, projected)


def solution(mesh):
    in_specs = (P("row", "gx", "gy"), P(None, "row", "gx", "gy"))
    out_specs = (P("gx", "gy"), P("gx", "gy"))
    return jax.shard_map(
        per_device, mesh=mesh, in_specs=in_specs, out_specs=out_specs, check_vma=False
    )
```

```python
import math

import jax
import jax.numpy as jnp
from jax import lax
from jax.experimental import pallas as pl
from jax.experimental.pallas import tpu as pltpu
from jax.sharding import PartitionSpec as P


BLOCK = 4
LEAP = 8

ADSORB = 0.6
HOPPING = 0.3
COUPLING = 0.5

LANES = 128
CHUNK = 8
GROUP = 16
F32 = jnp.float32
BF16 = jnp.bfloat16
MIB = 1 << 20


def iota(shape, dim):
    return lax.broadcasted_iota(jnp.int32, shape, dim)


def even_lanes(shape):
    return iota(shape, len(shape) - 1) % 2 == 0


def updated(centre, beside, draw):
    gone = 1.0 - jnp.exp2(beside * (-COUPLING * math.log2(math.e)))
    gain = ADSORB * draw
    keep = (1.0 - HOPPING - ADSORB) + (ADSORB - gain) * gone
    return centre * keep + (gain + (0.25 * HOPPING) * beside)


def fold_lanes(first):
    source = iota((LANES, LANES), 0)
    target = iota((LANES, LANES), 1)
    return selection(source // BLOCK + first == target)


def selection(picked):
    return jnp.where(picked, 1.0, 0.0).astype(BF16)


def split(x):
    high = x.astype(BF16)
    rest = x - high.astype(F32)
    middle = rest.astype(BF16)
    low = (rest - middle.astype(F32)).astype(BF16)
    return jnp.concatenate([high, middle, low])


def selected(x, matrix):
    size = x.shape[0]
    y = jnp.dot(split(x), matrix, preferred_element_type=F32)
    return (y[:size] + y[size : 2 * size]) + y[2 * size :]


def edges_kernel(occ, draws, low, high, obuf, dbuf, sems):
    reals, height, width = occ.shape
    copies = []
    for side, start in ((0, 0), (1, height - 8)):
        copies.append(
            pltpu.make_async_copy(occ.at[:, pl.ds(start, 8), :], obuf.at[side], sems.at[side, 0])
        )
        copies.append(
            pltpu.make_async_copy(
                draws.at[pl.ds(0, 3), :, pl.ds(start, 8), :], dbuf.at[side], sems.at[side, 1]
            )
        )
    for copy in copies:
        copy.start()
    even = even_lanes((8, LANES))
    row = iota((8, LANES), 0)
    even_row = row % 2 == 0

    def by_colour(x):
        swapped = jnp.where(even_row, pltpu.roll(x, 7, 0), pltpu.roll(x, 1, 0))
        return jnp.where(even, x, swapped)

    for side, out in ((0, low), (1, high)):
        copies[2 * side].wait()
        copies[2 * side + 1].wait()
        for r in range(reals):
            for c in range(width // LANES):
                lanes = slice(c * LANES, (c + 1) * LANES)
                first = by_colour(obuf[side, r, :, lanes].astype(F32))
                d0, d1, d2 = (
                    by_colour(dbuf[side, w, r, :, lanes].astype(F32)) for w in range(3)
                )
                mixed = pltpu.roll(jnp.where(even_row, d0, d1), 4, 0)
                if side == 0:
                    message = jnp.where(row < 4, first, jnp.where(row == 7, pltpu.roll(d2, 7, 0), mixed))
                else:
                    message = jnp.where(row >= 4, first, jnp.where(row == 1, pltpu.roll(d2, 3, 0), mixed))
                out[r, c] = message.astype(BF16)


def halo_rows(below, above, name):
    row = iota(below.shape, 0)
    moves = {
        "p0": ((2, 1), (0, 7)),
        "p1": ((1, 0), (7, 6)),
        "u0": ((6, 5), (4, 3)),
        "u1": ((4, 4), (3, 3)),
        "u2": ((6, 6), (1, 1)),
    }[name]
    (a6, a7), (b0, b1) = moves

    def moved(x, by):
        return x if by == 0 else pltpu.roll(x, by, 0)

    top = moved(above, a7) if a6 == a7 else jnp.where(row == 6, moved(above, a6), moved(above, a7))
    low = moved(below, b0) if b0 == b1 else jnp.where(row == 0, moved(below, b0), moved(below, b1))
    return top, low


NAMES = ("p0", "p1", "u0", "u1", "u2")


def tile_kernel(occ, draws, frames, strips, part, natural, state, sums):
    reals, height, width = occ.shape
    pairs = height // 2
    tiles = width // LANES
    sweeps = draws.shape[0]

    even = even_lanes((CHUNK, LANES))
    lane = iota((CHUNK, LANES), 1)
    sums[...] = jnp.zeros_like(sums)
    strips[...] = jnp.zeros_like(strips)
    for colour in range(2):
        for c in range(tiles):
            state[colour, c, 0:8] = jnp.zeros((8, LANES), F32)
            state[colour, c, pairs + 8 : pairs + 16] = jnp.zeros((8, LANES), F32)

    @pl.loop(0, reals)
    def _(r):
        group = lane // GROUP == r
        from_left = group & (lane % GROUP >= BLOCK)

        def keep_edges(index, c, value, start):
            if start == 0:
                frames[index, r, 0, c] = value[:8]
            if start == pairs - CHUNK:
                frames[index, r, 1, c] = value[CHUNK - 8 :]
            rows = slice(start, start + CHUNK)
            if c == 0:
                pltpu.store(strips.at[index, 0, rows], pltpu.roll(value, r * GROUP + BLOCK, 1), mask=from_left)
            if c == tiles - 1:
                pltpu.store(strips.at[index, 1, rows], pltpu.roll(value, r * GROUP + 12, 1), mask=group)

        for c in range(tiles):
            natural[sweeps, c] = occ[r, :, c * LANES : (c + 1) * LANES].astype(F32)
        for start in range(0, pairs, CHUNK):
            for c in range(tiles):
                first = natural[sweeps, c, pl.ds(2 * start, CHUNK, stride=2)]
                second = natural[sweeps, c, pl.ds(2 * start + 1, CHUNK, stride=2)]
                p0 = jnp.where(even, first, second)
                p1 = jnp.where(even, second, first)
                state[0, c, 8 + start : 8 + start + CHUNK] = p0
                state[1, c, 8 + start : 8 + start + CHUNK] = p1
                keep_edges(0, c, p0, start)
                keep_edges(1, c, p1, start)
        for w in range(sweeps):
            colour = w % 2
            other = 1 - colour
            for c in range(tiles):
                natural[w, c] = draws[w, r, :, c * LANES : (c + 1) * LANES].astype(F32)
            for start in range(0, pairs, CHUNK):
                heres = [state[other, c, 8 + start : 8 + start + CHUNK] for c in range(tiles)]
                for c in range(tiles):
                    first = natural[w, c, pl.ds(2 * start, CHUNK, stride=2)]
                    second = natural[w, c, pl.ds(2 * start + 1, CHUNK, stride=2)]
                    draw = jnp.where(even, first, second) if colour == 0 else jnp.where(even, second, first)
                    keep_edges(2 + w, c, draw, start)
                    here = heres[c]
                    up = state[other, c, 7 + start : 7 + start + CHUNK]
                    down = state[other, c, 9 + start : 9 + start + CHUNK]
                    vertical = jnp.where(even, up, down) if colour == 0 else jnp.where(even, down, up)
                    left = jnp.where(lane == LANES - 1, heres[(c - 1) % tiles], here)
                    right = jnp.where(lane == 0, heres[(c + 1) % tiles], here)
                    beside = pltpu.roll(left, 1, 1) + pltpu.roll(right, LANES - 1, 1)
                    new = updated(
                        state[colour, c, 8 + start : 8 + start + CHUNK], (here + vertical) + beside, draw
                    )
                    state[colour, c, 8 + start : 8 + start + CHUNK] = new
                    if w == sweeps - 3 or w == sweeps - 1:
                        snapshot = 0 if w == sweeps - 3 else 1
                        sums[snapshot, c, start : start + CHUNK] += here + new

    half = pairs // 2
    total = jnp.zeros((2 * half, LANES), F32)
    for c in range(tiles):
        rows = jnp.concatenate(
            [
                sums[s, c, pl.ds(0, half, stride=2)] + sums[s, c, pl.ds(1, half, stride=2)]
                for s in range(2)
            ]
        )
        total += selected(rows, fold_lanes(c * (LANES // BLOCK)))
    part[0] = total[:half]
    part[1] = total[half:]


def strips_kernel(below, above, strips, message, corners):
    reals, tiles = below.shape[:2]
    pairs = strips.shape[2]
    lane = iota((8, LANES), 1)
    for v, source in ((0, above), (1, below)):
        sides = [jnp.zeros((8, LANES), F32) for _ in range(2)]
        for r in range(reals):
            group = lane // GROUP == r
            left = pltpu.roll(source[r, 0].astype(F32), r * GROUP + BLOCK, 1)
            right = pltpu.roll(source[r, tiles - 1].astype(F32), (r * GROUP + 12) % LANES, 1)
            sides[0] = jnp.where(group & (lane % GROUP >= BLOCK), left, sides[0])
            sides[1] = jnp.where(group, right, sides[1])
        corners[0, v] = sides[0]
        corners[1, v] = sides[1]
        message[len(NAMES) * pairs + 8 * v : len(NAMES) * pairs + 8 * v + 8] = jnp.where(
            lane % GROUP < 8, sides[0], sides[1]
        ).astype(BF16)
    lane = iota((pairs, LANES), 1)
    for index in range(len(NAMES)):
        message[index * pairs : (index + 1) * pairs] = jnp.where(
            lane % GROUP < 8, strips[index, 0], strips[index, 1]
        ).astype(BF16)


def rows_kernel(below, above, frames, out, arrays):
    reals, tiles = below.shape[:2]
    sweeps = frames.shape[0] - 2
    even = even_lanes((8, LANES))
    lane = iota((8, LANES), 1)
    row = iota((8, LANES), 0)
    sides = range(2)
    for r in range(reals):
        for c in range(tiles):
            low = below[r, c].astype(F32)
            high = above[r, c].astype(F32)
            for index, name in enumerate(NAMES):
                top, bottom = halo_rows(low, high, name)
                arrays[index, r, 0, c] = jnp.where(row >= 6, top, frames[index, r, 0, c])
                arrays[index, r, 1, c] = jnp.where(row < 2, bottom, frames[index, r, 1, c])
    sums = [[[None] * tiles for _ in sides] for _ in range(2)]
    for w in range(sweeps):
        colour = w % 2
        other = 1 - colour
        for r in range(reals):
            for side in sides:
                for c in range(tiles):
                    draw = arrays[2 + w, r, side, c] if w < 3 else frames[2 + w, r, side, c]
                    here = arrays[other, r, side, c]
                    up = pltpu.roll(here, 1, 0)
                    down = pltpu.roll(here, 7, 0)
                    vertical = jnp.where(even, up, down) if colour == 0 else jnp.where(even, down, up)
                    left = arrays[other, r, side, (c - 1) % tiles]
                    right = arrays[other, r, side, (c + 1) % tiles]
                    left = pltpu.roll(jnp.where(lane == LANES - 1, left, here), 1, 1)
                    right = pltpu.roll(jnp.where(lane == 0, right, here), LANES - 1, 1)
                    new = updated(
                        arrays[colour, r, side, c], (here + vertical) + (left + right), draw
                    )
                    arrays[colour, r, side, c] = new
                    if w == sweeps - 3 or w == sweeps - 1:
                        s = 0 if w == sweeps - 3 else 1
                        both = here + new
                        before = sums[s][side][c]
                        sums[s][side][c] = both if before is None else before + both
    total = jnp.zeros((8, LANES), F32)
    for c in range(tiles):
        rows = jnp.zeros((8, LANES), F32)
        for s in range(2):
            for side in sides:
                both = sums[s][side][c]
                both = both + pltpu.roll(both, 1, 0)
                index = 2 * s + side
                shift = (index - (1 if side == 0 else 7)) % 8
                both = both if shift == 0 else pltpu.roll(both, shift, 0)
                rows = jnp.where(row == index, both, rows)
        total += selected(rows, fold_lanes(c * (LANES // BLOCK)))
    out[...] = total


def columns_kernel(strips, corners, from_left, from_right, part, rows, out, arrays):
    pairs = strips.shape[2]
    sweeps = strips.shape[0] - 2
    base = 16
    count = len(NAMES)
    lane = iota((pairs, LANES), 1) % GROUP
    lane8 = iota((8, LANES), 1) % GROUP
    row8 = iota((8, LANES), 0)

    def joined(side, q, own, left, right):
        if side == 0:
            return jnp.where(q < BLOCK, pltpu.roll(left, LANES - 8, 1), own)
        return jnp.where(q >= GROUP - BLOCK, pltpu.roll(right, 8, 1), own)

    zero = jnp.zeros((8, LANES), F32)
    for side in range(2):
        for index in range(count):
            rows_of = slice(index * pairs, (index + 1) * pairs)
            arrays[index, side, base : base + pairs] = joined(
                side, lane, strips[index, side], from_left[rows_of].astype(F32), from_right[rows_of].astype(F32)
            )
        halos = []
        for v in range(2):
            rows_of = slice(count * pairs + 8 * v, count * pairs + 8 * v + 8)
            halos.append(
                joined(side, lane8, corners[side, v], from_left[rows_of].astype(F32), from_right[rows_of].astype(F32))
            )
        for index, name in enumerate(NAMES):
            top, bottom = halo_rows(halos[1], halos[0], name)
            arrays[index, side, base - 8 : base] = jnp.where(row8 >= 6, top, 0.0)
            arrays[index, side, base + pairs : base + pairs + 8] = jnp.where(row8 < 2, bottom, 0.0)
            if index < 2:
                arrays[index, side, 0 : base - 8] = zero
                arrays[index, side, base + pairs + 8 : base + pairs + 16] = zero
        arrays[count, side, base : base + pairs] = strips[count, side]
        arrays[count, side, base - 8 : base] = zero
        arrays[count, side, base + pairs : base + pairs + 8] = zero
    half = pairs // 2
    for w in range(sweeps):
        colour = w % 2
        other = 1 - colour
        grow = 8 if w < sweeps - 1 else 0
        start, size = base - grow, pairs + 2 * grow
        even = even_lanes((size, LANES))
        for side in range(2):
            here = arrays[other, side, start : start + size]
            up = arrays[other, side, start - 1 : start - 1 + size]
            down = arrays[other, side, start + 1 : start + 1 + size]
            vertical = jnp.where(even, up, down) if colour == 0 else jnp.where(even, down, up)
            beside = (here + vertical) + (pltpu.roll(here, 1, 1) + pltpu.roll(here, LANES - 1, 1))
            new = updated(
                arrays[colour, side, start : start + size], beside, arrays[2 + w, side, start : start + size]
            )
            arrays[colour, side, start : start + size] = new
            if w == sweeps - 3 or w == sweeps - 1:
                s = 0 if w == sweeps - 3 else 1
                arrays[count + 1 + s, side, base : base + pairs] = (here + new)[grow : grow + pairs]
    source = iota((LANES, LANES), 0) % GROUP
    target = iota((LANES, LANES), 1)
    total = jnp.zeros((2 * half, LANES), F32)
    for side in range(2):
        rows_of = jnp.concatenate(
            [
                arrays[count + 1 + s, side, pl.ds(base, half, stride=2)]
                + arrays[count + 1 + s, side, pl.ds(base + 1, half, stride=2)]
                for s in range(2)
            ]
        )
        first = BLOCK if side == 0 else 2 * BLOCK
        pick = (source >= first) & (source < first + BLOCK) & (target == (0 if side == 0 else LANES - 1))
        total += selected(rows_of, selection(pick))
    row = iota((half, LANES), 0)
    column = iota((half, LANES), 1)
    for s in range(2):
        value = part[s]
        value = jnp.where(row == 0, rows[2 * s : 2 * s + 1], value)
        value = jnp.where(row == half - 1, rows[2 * s + 1 : 2 * s + 2], value)
        edge = (column == 0) | (column == LANES - 1)
        out[s] = jnp.where(edge, total[s * half : (s + 1) * half], value)


def shifted(value, axis, by):
    count = lax.axis_size(axis)
    if count == 1:
        return value
    return lax.ppermute(value, axis, [(i, (i + by) % count) for i in range(count)])


def both_ways(to_low, to_high, axis):
    before = shifted(to_high, axis, 1)
    after = shifted(to_low, axis, -1)
    return after, before


def call(kernel, args, outs, vmem, scratch=(), flops=0, space=pltpu.VMEM):
    if space == pltpu.HBM:
        args = [pltpu.with_memory_space_constraint(arg, space) for arg in args]
    return pl.pallas_call(
        kernel,
        out_shape=tuple(pltpu.VMEM(shape, dtype) for shape, dtype in outs),
        in_specs=[pl.BlockSpec(memory_space=space) for _ in args],
        out_specs=tuple(pl.BlockSpec(memory_space=pltpu.VMEM) for _ in outs),
        scratch_shapes=list(scratch),
        compiler_params=pltpu.CompilerParams(vmem_limit_bytes=vmem * MIB),
        cost_estimate=pl.CostEstimate(flops=flops, bytes_accessed=0, transcendentals=0),
    )(*args)


def integrated(occupancy, random_draws):
    reals, height, width = occupancy.shape
    sweeps = random_draws.shape[0]
    tiles, pairs, half = width // LANES, height // 2, height // BLOCK
    edge = ((reals, tiles, 8, LANES), BF16)
    low, high = call(
        edges_kernel,
        (occupancy, random_draws),
        (edge, edge),
        8,
        (
            pltpu.VMEM((2, reals, 8, width), jnp.int32),
            pltpu.VMEM((2, 3, reals, 8, width), BF16),
            pltpu.SemaphoreType.DMA((2, 2)),
        ),
        1_000_000,
        pltpu.HBM,
    )
    below, above = both_ways(low, high, "gx")
    frames, strips, part = call(
        tile_kernel,
        (occupancy, random_draws),
        (
            ((2 + sweeps, reals, 2, tiles, 8, LANES), F32),
            ((2 + sweeps, 2, pairs, LANES), F32),
            ((2, half, LANES), F32),
        ),
        24,
        (
            pltpu.VMEM((sweeps + 1, tiles, height, LANES), F32),
            pltpu.VMEM((2, tiles, pairs + 16, LANES), F32),
            pltpu.VMEM((2, tiles, pairs, LANES), F32),
        ),
        40_000_000,
    )
    message, corners = call(
        strips_kernel,
        (below, above, strips),
        (((len(NAMES) * pairs + 16, LANES), BF16), ((2, 2, 8, LANES), F32)),
        4,
        (),
        1_000_000,
    )
    if lax.axis_size("gy") == 2:
        from_left = from_right = shifted(message, "gy", 1)
    else:
        from_right, from_left = both_ways(message, message, "gy")
    (rows,) = call(
        rows_kernel,
        (below, above, frames),
        (((8, LANES), F32),),
        8,
        (pltpu.VMEM((len(NAMES), reals, 2, tiles, 8, LANES), F32),),
        10_000_000,
    )
    (mine,) = call(
        columns_kernel,
        (strips, corners, from_left, from_right, part, rows),
        (((2, half, LANES), F32),),
        8,
        (pltpu.VMEM((len(NAMES) + 3, 2, pairs + 32, LANES), F32),),
        4_000_000,
    )
    count = lax.axis_size("row")
    if count == 4:
        theirs = {}
        for other in (1, 2, 3):
            theirs[other] = lax.ppermute(mine, "row", [(i, i ^ other) for i in range(count)])
        coarse_sums = (mine + theirs[2]) + (theirs[1] + theirs[3])
    else:
        coarse_sums = lax.psum(mine, "row")
    averages = coarse_sums * jnp.float32(1.0 / (reals * count * BLOCK * BLOCK))
    coverage = averages[1]
    projected = coverage + LEAP / 2.0 * (coverage - averages[0])
    return (coverage, projected)


def solution(mesh):
    in_specs = (P("row", "gx", "gy"), P(None, "row", "gx", "gy"))
    out_specs = (P("gx", "gy"), P("gx", "gy"))
    return jax.shard_map(integrated, mesh=mesh, in_specs=in_specs, out_specs=out_specs, check_vma=False)
```

```python
import math

import jax
import jax.numpy as jnp
from jax import lax
from jax.experimental import pallas as pl
from jax.experimental.pallas import tpu as pltpu
from jax.sharding import PartitionSpec as P


BLOCK = 4
LEAP = 8

ADSORB = 0.6
HOPPING = 0.3
COUPLING = 0.5

LANES = 128
CHUNK = 8
GROUP = 16
F32 = jnp.float32
BF16 = jnp.bfloat16
MIB = 1 << 20


def iota(shape, dim):
    return lax.broadcasted_iota(jnp.int32, shape, dim)


def even_lanes(shape):
    return iota(shape, len(shape) - 1) % 2 == 0


def updated(centre, beside, draw):
    gone = 1.0 - jnp.exp2(beside * (-COUPLING * math.log2(math.e)))
    gain = ADSORB * draw
    keep = (1.0 - HOPPING - ADSORB) + (ADSORB - gain) * gone
    return centre * keep + (gain + (0.25 * HOPPING) * beside)


def fold_lanes(first):
    source = iota((LANES, LANES), 0)
    target = iota((LANES, LANES), 1)
    return selection(source // BLOCK + first == target)


def selection(picked):
    return jnp.where(picked, 1.0, 0.0).astype(BF16)


def split(x):
    high = x.astype(BF16)
    rest = x - high.astype(F32)
    middle = rest.astype(BF16)
    low = (rest - middle.astype(F32)).astype(BF16)
    return jnp.concatenate([high, middle, low])


def selected(x, matrix):
    size = x.shape[0]
    y = jnp.dot(split(x), matrix, preferred_element_type=F32)
    return (y[:size] + y[size : 2 * size]) + y[2 * size :]


def edges_kernel(occ, draws, low, high, obuf, dbuf, sems):
    reals, height, width = occ.shape
    copies = []
    for side, start in ((0, 0), (1, height - 8)):
        copies.append(
            pltpu.make_async_copy(occ.at[:, pl.ds(start, 8), :], obuf.at[side], sems.at[side, 0])
        )
        copies.append(
            pltpu.make_async_copy(
                draws.at[pl.ds(0, 3), :, pl.ds(start, 8), :], dbuf.at[side], sems.at[side, 1]
            )
        )
    for copy in copies:
        copy.start()
    even = even_lanes((8, LANES))
    row = iota((8, LANES), 0)
    even_row = row % 2 == 0

    def by_colour(x):
        swapped = jnp.where(even_row, pltpu.roll(x, 7, 0), pltpu.roll(x, 1, 0))
        return jnp.where(even, x, swapped)

    for side, out in ((0, low), (1, high)):
        copies[2 * side].wait()
        copies[2 * side + 1].wait()
        for r in range(reals):
            for c in range(width // LANES):
                lanes = slice(c * LANES, (c + 1) * LANES)
                first = by_colour(obuf[side, r, :, lanes].astype(F32))
                d0, d1, d2 = (
                    by_colour(dbuf[side, w, r, :, lanes].astype(F32)) for w in range(3)
                )
                mixed = pltpu.roll(jnp.where(even_row, d0, d1), 4, 0)
                if side == 0:
                    message = jnp.where(row < 4, first, jnp.where(row == 7, pltpu.roll(d2, 7, 0), mixed))
                else:
                    message = jnp.where(row >= 4, first, jnp.where(row == 1, pltpu.roll(d2, 3, 0), mixed))
                out[r, c] = message.astype(BF16)


def halo_rows(below, above, name):
    row = iota(below.shape, 0)
    moves = {
        "p0": ((2, 1), (0, 7)),
        "p1": ((1, 0), (7, 6)),
        "u0": ((6, 5), (4, 3)),
        "u1": ((4, 4), (3, 3)),
        "u2": ((6, 6), (1, 1)),
    }[name]
    (a6, a7), (b0, b1) = moves

    def moved(x, by):
        return x if by == 0 else pltpu.roll(x, by, 0)

    top = moved(above, a7) if a6 == a7 else jnp.where(row == 6, moved(above, a6), moved(above, a7))
    low = moved(below, b0) if b0 == b1 else jnp.where(row == 0, moved(below, b0), moved(below, b1))
    return top, low


NAMES = ("p0", "p1", "u0", "u1", "u2")


def tile_kernel(occ, draws, frames, strips, sums, natural, state):
    reals, height, width = occ.shape
    pairs = height // 2
    tiles = width // LANES
    sweeps = draws.shape[0]

    even = even_lanes((CHUNK, LANES))
    lane = iota((CHUNK, LANES), 1)
    sums[...] = jnp.zeros_like(sums)
    strips[...] = jnp.zeros_like(strips)
    for colour in range(2):
        for c in range(tiles):
            for i in range(2):
                state[i, colour, c, 0:8] = jnp.zeros((8, LANES), F32)
                state[i, colour, c, pairs + 8 : pairs + 16] = jnp.zeros((8, LANES), F32)

    def one(r, natural, state):
        group = lane // GROUP == r
        from_left = group & (lane % GROUP >= BLOCK)

        def keep_edges(index, c, value, start):
            if start == 0:
                frames[index, r, 0, c] = value[:8]
            if start == pairs - CHUNK:
                frames[index, r, 1, c] = value[CHUNK - 8 :]
            rows = slice(start, start + CHUNK)
            if c == 0:
                pltpu.store(strips.at[index, 0, rows], pltpu.roll(value, r * GROUP + BLOCK, 1), mask=from_left)
            if c == tiles - 1:
                pltpu.store(strips.at[index, 1, rows], pltpu.roll(value, r * GROUP + 12, 1), mask=group)

        for c in range(tiles):
            natural[sweeps, c, :height] = occ[r, :, c * LANES : (c + 1) * LANES].astype(F32)
        for start in range(0, pairs, CHUNK):
            for c in range(tiles):
                first = natural[sweeps, c, pl.ds(2 * start, CHUNK, stride=2)]
                second = natural[sweeps, c, pl.ds(2 * start + 1, CHUNK, stride=2)]
                p0 = jnp.where(even, first, second)
                p1 = jnp.where(even, second, first)
                state[0, c, 8 + start : 8 + start + CHUNK] = p0
                state[1, c, 8 + start : 8 + start + CHUNK] = p1
                keep_edges(0, c, p0, start)
                keep_edges(1, c, p1, start)
        for w in range(sweeps):
            colour = w % 2
            other = 1 - colour
            for c in range(tiles):
                natural[w, c, :height] = draws[w, r, :, c * LANES : (c + 1) * LANES].astype(F32)
            for start in range(0, pairs, CHUNK):
                heres = [state[other, c, 8 + start : 8 + start + CHUNK] for c in range(tiles)]
                for c in range(tiles):
                    first = natural[w, c, pl.ds(2 * start, CHUNK, stride=2)]
                    second = natural[w, c, pl.ds(2 * start + 1, CHUNK, stride=2)]
                    draw = jnp.where(even, first, second) if colour == 0 else jnp.where(even, second, first)
                    keep_edges(2 + w, c, draw, start)
                    here = heres[c]
                    up = state[other, c, 7 + start : 7 + start + CHUNK]
                    down = state[other, c, 9 + start : 9 + start + CHUNK]
                    vertical = jnp.where(even, up, down) if colour == 0 else jnp.where(even, down, up)
                    left = jnp.where(lane == LANES - 1, heres[(c - 1) % tiles], here)
                    right = jnp.where(lane == 0, heres[(c + 1) % tiles], here)
                    beside = pltpu.roll(left, 1, 1) + pltpu.roll(right, LANES - 1, 1)
                    new = updated(
                        state[colour, c, 8 + start : 8 + start + CHUNK], (here + vertical) + beside, draw
                    )
                    state[colour, c, 8 + start : 8 + start + CHUNK] = new
                    if w == sweeps - 3 or w == sweeps - 1:
                        snapshot = 0 if w == sweeps - 3 else 1
                        sums[snapshot, c, start : start + CHUNK] += here + new

    together = 2 if reals % 2 == 0 else 1

    @pl.loop(0, reals // together)
    def _(step):
        for i in range(together):
            one(step * together + i, natural.at[i], state.at[i])


def strips_kernel(below, above, strips, message, corners):
    reals, tiles = below.shape[:2]
    pairs = strips.shape[2]
    lane = iota((8, LANES), 1)
    for v, source in ((0, above), (1, below)):
        sides = [jnp.zeros((8, LANES), F32) for _ in range(2)]
        for r in range(reals):
            group = lane // GROUP == r
            left = pltpu.roll(source[r, 0].astype(F32), r * GROUP + BLOCK, 1)
            right = pltpu.roll(source[r, tiles - 1].astype(F32), (r * GROUP + 12) % LANES, 1)
            sides[0] = jnp.where(group & (lane % GROUP >= BLOCK), left, sides[0])
            sides[1] = jnp.where(group, right, sides[1])
        corners[0, v] = sides[0]
        corners[1, v] = sides[1]
        message[len(NAMES) * pairs + 8 * v : len(NAMES) * pairs + 8 * v + 8] = jnp.where(
            lane % GROUP < 8, sides[0], sides[1]
        ).astype(BF16)
    lane = iota((pairs, LANES), 1)
    for index in range(len(NAMES)):
        message[index * pairs : (index + 1) * pairs] = jnp.where(
            lane % GROUP < 8, strips[index, 0], strips[index, 1]
        ).astype(BF16)


def rows_kernel(below, above, frames, inner, out, arrays):
    reals, tiles = below.shape[:2]
    sweeps = frames.shape[0] - 2
    even = even_lanes((8, LANES))
    lane = iota((8, LANES), 1)
    row = iota((8, LANES), 0)
    sides = range(2)
    for r in range(reals):
        for c in range(tiles):
            low = below[r, c].astype(F32)
            high = above[r, c].astype(F32)
            for index, name in enumerate(NAMES):
                top, bottom = halo_rows(low, high, name)
                arrays[index, r, 0, c] = jnp.where(row >= 6, top, frames[index, r, 0, c])
                arrays[index, r, 1, c] = jnp.where(row < 2, bottom, frames[index, r, 1, c])
    sums = [[[None] * tiles for _ in sides] for _ in range(2)]
    for w in range(sweeps):
        colour = w % 2
        other = 1 - colour
        for r in range(reals):
            for side in sides:
                for c in range(tiles):
                    draw = arrays[2 + w, r, side, c] if w < 3 else frames[2 + w, r, side, c]
                    here = arrays[other, r, side, c]
                    up = pltpu.roll(here, 1, 0)
                    down = pltpu.roll(here, 7, 0)
                    vertical = jnp.where(even, up, down) if colour == 0 else jnp.where(even, down, up)
                    left = arrays[other, r, side, (c - 1) % tiles]
                    right = arrays[other, r, side, (c + 1) % tiles]
                    left = pltpu.roll(jnp.where(lane == LANES - 1, left, here), 1, 1)
                    right = pltpu.roll(jnp.where(lane == 0, right, here), LANES - 1, 1)
                    new = updated(
                        arrays[colour, r, side, c], (here + vertical) + (left + right), draw
                    )
                    arrays[colour, r, side, c] = new
                    if w == sweeps - 3 or w == sweeps - 1:
                        s = 0 if w == sweeps - 3 else 1
                        both = here + new
                        before = sums[s][side][c]
                        sums[s][side][c] = both if before is None else before + both
    half = inner.shape[2] // 2
    total = jnp.zeros((2 * half, LANES), F32)
    for c in range(tiles):
        lines = []
        for s in range(2):
            cells = inner[s, c, pl.ds(0, half, stride=2)] + inner[s, c, pl.ds(1, half, stride=2)]
            top, bottom = sums[s][0][c], sums[s][1][c]
            lines.append(jnp.where(row == 0, top + pltpu.roll(top, 7, 0), cells[:8]))
            lines.append(cells[8 : half - 8])
            lines.append(jnp.where(row == 7, bottom + pltpu.roll(bottom, 1, 0), cells[half - 8 :]))
        total += selected(jnp.concatenate(lines), fold_lanes(c * (LANES // BLOCK)))
    out[0] = total[:half]
    out[1] = total[half:]


def columns_kernel(strips, corners, from_left, from_right, part, out, arrays):
    pairs = strips.shape[2]
    sweeps = strips.shape[0] - 2
    base = 16
    count = len(NAMES)
    lane = iota((pairs, LANES), 1) % GROUP
    lane8 = iota((8, LANES), 1) % GROUP
    row8 = iota((8, LANES), 0)

    def joined(side, q, own, left, right):
        if side == 0:
            return jnp.where(q < BLOCK, pltpu.roll(left, LANES - 8, 1), own)
        return jnp.where(q >= GROUP - BLOCK, pltpu.roll(right, 8, 1), own)

    zero = jnp.zeros((8, LANES), F32)
    for side in range(2):
        for index in range(count):
            rows_of = slice(index * pairs, (index + 1) * pairs)
            arrays[index, side, base : base + pairs] = joined(
                side, lane, strips[index, side], from_left[rows_of].astype(F32), from_right[rows_of].astype(F32)
            )
        halos = []
        for v in range(2):
            rows_of = slice(count * pairs + 8 * v, count * pairs + 8 * v + 8)
            halos.append(
                joined(side, lane8, corners[side, v], from_left[rows_of].astype(F32), from_right[rows_of].astype(F32))
            )
        for index, name in enumerate(NAMES):
            top, bottom = halo_rows(halos[1], halos[0], name)
            arrays[index, side, base - 8 : base] = jnp.where(row8 >= 6, top, 0.0)
            arrays[index, side, base + pairs : base + pairs + 8] = jnp.where(row8 < 2, bottom, 0.0)
            if index < 2:
                arrays[index, side, 0 : base - 8] = zero
                arrays[index, side, base + pairs + 8 : base + pairs + 16] = zero
        arrays[count, side, base : base + pairs] = strips[count, side]
        arrays[count, side, base - 8 : base] = zero
        arrays[count, side, base + pairs : base + pairs + 8] = zero
    half = pairs // 2
    for w in range(sweeps):
        colour = w % 2
        other = 1 - colour
        grow = 8 if w < sweeps - 1 else 0
        start, size = base - grow, pairs + 2 * grow
        even = even_lanes((size, LANES))
        for side in range(2):
            here = arrays[other, side, start : start + size]
            up = arrays[other, side, start - 1 : start - 1 + size]
            down = arrays[other, side, start + 1 : start + 1 + size]
            vertical = jnp.where(even, up, down) if colour == 0 else jnp.where(even, down, up)
            beside = (here + vertical) + (pltpu.roll(here, 1, 1) + pltpu.roll(here, LANES - 1, 1))
            new = updated(
                arrays[colour, side, start : start + size], beside, arrays[2 + w, side, start : start + size]
            )
            arrays[colour, side, start : start + size] = new
            if w == sweeps - 3 or w == sweeps - 1:
                s = 0 if w == sweeps - 3 else 1
                arrays[count + 1 + s, side, base : base + pairs] = (here + new)[grow : grow + pairs]
    column = iota((half, LANES), 1)
    group = column % GROUP
    for s in range(2):
        value = part[s]
        for side in range(2):
            cells = (
                arrays[count + 1 + s, side, pl.ds(base, half, stride=2)]
                + arrays[count + 1 + s, side, pl.ds(base + 1, half, stride=2)]
            )
            first = BLOCK if side == 0 else 2 * BLOCK
            own = jnp.where((group >= first) & (group < first + BLOCK), cells, 0.0)
            sums = jnp.sum(own, axis=1, keepdims=True)
            value = jnp.where(column == (0 if side == 0 else LANES - 1), sums, value)
        out[s] = value


def shifted(value, axis, by):
    count = lax.axis_size(axis)
    if count == 1:
        return value
    return lax.ppermute(value, axis, [(i, (i + by) % count) for i in range(count)])


def both_ways(to_low, to_high, axis):
    before = shifted(to_high, axis, 1)
    after = shifted(to_low, axis, -1)
    return after, before


def call(kernel, args, outs, vmem, scratch=(), flops=0, space=pltpu.VMEM):
    if space == pltpu.HBM:
        args = [pltpu.with_memory_space_constraint(arg, space) for arg in args]
    return pl.pallas_call(
        kernel,
        out_shape=tuple(pltpu.VMEM(shape, dtype) for shape, dtype in outs),
        in_specs=[pl.BlockSpec(memory_space=space) for _ in args],
        out_specs=tuple(pl.BlockSpec(memory_space=pltpu.VMEM) for _ in outs),
        scratch_shapes=list(scratch),
        compiler_params=pltpu.CompilerParams(vmem_limit_bytes=vmem * MIB),
        cost_estimate=pl.CostEstimate(flops=flops, bytes_accessed=0, transcendentals=0),
    )(*args)


def integrated(occupancy, random_draws):
    reals, height, width = occupancy.shape
    sweeps = random_draws.shape[0]
    tiles, pairs, half = width // LANES, height // 2, height // BLOCK
    edge = ((reals, tiles, 8, LANES), BF16)
    low, high = call(
        edges_kernel,
        (occupancy, random_draws),
        (edge, edge),
        8,
        (
            pltpu.VMEM((2, reals, 8, width), jnp.int32),
            pltpu.VMEM((2, 3, reals, 8, width), BF16),
            pltpu.SemaphoreType.DMA((2, 2)),
        ),
        1_000_000,
        pltpu.HBM,
    )
    below, above = both_ways(low, high, "gx")
    frames, strips, inner = call(
        tile_kernel,
        (occupancy, random_draws),
        (
            ((2 + sweeps, reals, 2, tiles, 8, LANES), F32),
            ((2 + sweeps, 2, pairs, LANES), F32),
            ((2, tiles, pairs, LANES), F32),
        ),
        24,
        (
            pltpu.VMEM((2, sweeps + 1, tiles, height + 8, LANES), F32),
            pltpu.VMEM((2, 2, tiles, pairs + 16, LANES), F32),
        ),
        40_000_000,
    )
    message, corners = call(
        strips_kernel,
        (below, above, strips),
        (((len(NAMES) * pairs + 16, LANES), BF16), ((2, 2, 8, LANES), F32)),
        4,
        (),
        1_000_000,
    )
    if lax.axis_size("gy") == 2:
        from_left = from_right = shifted(message, "gy", 1)
    else:
        from_right, from_left = both_ways(message, message, "gy")
    (part,) = call(
        rows_kernel,
        (below, above, frames, inner),
        (((2, half, LANES), F32),),
        8,
        (pltpu.VMEM((len(NAMES), reals, 2, tiles, 8, LANES), F32),),
        10_000_000,
    )
    (mine,) = call(
        columns_kernel,
        (strips, corners, from_left, from_right, part),
        (((2, half, LANES), F32),),
        8,
        (pltpu.VMEM((len(NAMES) + 3, 2, pairs + 32, LANES), F32),),
        4_000_000,
    )
    count = lax.axis_size("row")
    if count == 4:
        theirs = {}
        for other in (1, 2, 3):
            theirs[other] = lax.ppermute(mine, "row", [(i, i ^ other) for i in range(count)])
        coarse_sums = (mine + theirs[2]) + (theirs[1] + theirs[3])
    else:
        coarse_sums = lax.psum(mine, "row")
    averages = coarse_sums * jnp.float32(1.0 / (reals * count * BLOCK * BLOCK))
    coverage = averages[1]
    projected = coverage + LEAP / 2.0 * (coverage - averages[0])
    return (coverage, projected)


def solution(mesh):
    in_specs = (P("row", "gx", "gy"), P(None, "row", "gx", "gy"))
    out_specs = (P("gx", "gy"), P("gx", "gy"))
    return jax.shard_map(integrated, mesh=mesh, in_specs=in_specs, out_specs=out_specs, check_vma=False)
```

```python
import math

import jax
import jax.numpy as jnp
from jax import lax
from jax.experimental import pallas as pl
from jax.experimental.pallas import tpu as pltpu
from jax.sharding import PartitionSpec as P


BLOCK = 4
LEAP = 8

ADSORB = 0.6
HOPPING = 0.3
COUPLING = 0.5

LANES = 128
CHUNK = 8
GROUP = 16
F32 = jnp.float32
BF16 = jnp.bfloat16
MIB = 1 << 20


def iota(shape, dim):
    return lax.broadcasted_iota(jnp.int32, shape, dim)


def even_lanes(shape):
    return iota(shape, len(shape) - 1) % 2 == 0


def updated(centre, beside, draw):
    gone = 1.0 - jnp.exp2(beside * (-COUPLING * math.log2(math.e)))
    gain = ADSORB * draw
    keep = (1.0 - HOPPING - ADSORB) + (ADSORB - gain) * gone
    return centre * keep + (gain + (0.25 * HOPPING) * beside)


def fold_lanes(first):
    source = iota((LANES, LANES), 0)
    target = iota((LANES, LANES), 1)
    return selection(source // BLOCK + first == target)


def selection(picked):
    return jnp.where(picked, 1.0, 0.0).astype(BF16)


def split(x):
    high = x.astype(BF16)
    rest = x - high.astype(F32)
    middle = rest.astype(BF16)
    low = (rest - middle.astype(F32)).astype(BF16)
    return jnp.concatenate([high, middle, low])


def selected(x, matrix):
    size = x.shape[0]
    y = jnp.dot(split(x), matrix, preferred_element_type=F32)
    return (y[:size] + y[size : 2 * size]) + y[2 * size :]


def edges_kernel(occ, draws, low, high, obuf, dbuf, sems):
    reals, height, width = occ.shape
    copies = []
    for side, start in ((0, 0), (1, height - 8)):
        copies.append(
            pltpu.make_async_copy(occ.at[:, pl.ds(start, 8), :], obuf.at[side], sems.at[side, 0])
        )
        copies.append(
            pltpu.make_async_copy(
                draws.at[pl.ds(0, 3), :, pl.ds(start, 8), :], dbuf.at[side], sems.at[side, 1]
            )
        )
    for copy in copies:
        copy.start()
    even = even_lanes((8, LANES))
    row = iota((8, LANES), 0)
    even_row = row % 2 == 0

    def by_colour(x):
        swapped = jnp.where(even_row, pltpu.roll(x, 7, 0), pltpu.roll(x, 1, 0))
        return jnp.where(even, x, swapped)

    for side, out in ((0, low), (1, high)):
        copies[2 * side].wait()
        copies[2 * side + 1].wait()
        for r in range(reals):
            for c in range(width // LANES):
                lanes = slice(c * LANES, (c + 1) * LANES)
                first = by_colour(obuf[side, r, :, lanes].astype(F32))
                d0, d1, d2 = (
                    by_colour(dbuf[side, w, r, :, lanes].astype(F32)) for w in range(3)
                )
                mixed = pltpu.roll(jnp.where(even_row, d0, d1), 4, 0)
                if side == 0:
                    message = jnp.where(row < 4, first, jnp.where(row == 7, pltpu.roll(d2, 7, 0), mixed))
                else:
                    message = jnp.where(row >= 4, first, jnp.where(row == 1, pltpu.roll(d2, 3, 0), mixed))
                out[r, c] = message.astype(BF16)


def halo_rows(below, above, name):
    row = iota(below.shape, 0)
    moves = {
        "p0": ((2, 1), (0, 7)),
        "p1": ((1, 0), (7, 6)),
        "u0": ((6, 5), (4, 3)),
        "u1": ((4, 4), (3, 3)),
        "u2": ((6, 6), (1, 1)),
    }[name]
    (a6, a7), (b0, b1) = moves

    def moved(x, by):
        return x if by == 0 else pltpu.roll(x, by, 0)

    top = moved(above, a7) if a6 == a7 else jnp.where(row == 6, moved(above, a6), moved(above, a7))
    low = moved(below, b0) if b0 == b1 else jnp.where(row == 0, moved(below, b0), moved(below, b1))
    return top, low


NAMES = ("p0", "p1", "u0", "u1", "u2")


def tile_kernel(occ, draws, frames, strips, sums, natural, state):
    reals, height, width = occ.shape
    pairs = height // 2
    tiles = width // LANES
    sweeps = draws.shape[0]

    even = even_lanes((CHUNK, LANES))
    lane = iota((CHUNK, LANES), 1)
    sums[...] = jnp.zeros_like(sums)
    strips[...] = jnp.zeros_like(strips)
    for colour in range(2):
        for c in range(tiles):
            for i in range(2):
                state[i, colour, c, 0:8] = jnp.zeros((8, LANES), F32)
                state[i, colour, c, pairs + 8 : pairs + 16] = jnp.zeros((8, LANES), F32)

    def one(r, natural, state):
        group = lane // GROUP == r
        from_left = group & (lane % GROUP >= BLOCK)

        def keep_edges(index, c, value, start):
            if start == 0:
                frames[index, r, 0, c] = value[:8]
            if start == pairs - CHUNK:
                frames[index, r, 1, c] = value[CHUNK - 8 :]
            rows = slice(start, start + CHUNK)
            if c == 0:
                pltpu.store(strips.at[index, 0, rows], pltpu.roll(value, r * GROUP + BLOCK, 1), mask=from_left)
            if c == tiles - 1:
                pltpu.store(strips.at[index, 1, rows], pltpu.roll(value, r * GROUP + 12, 1), mask=group)

        for c in range(tiles):
            natural[sweeps, c, :height] = occ[r, :, c * LANES : (c + 1) * LANES].astype(F32)
        for start in range(0, pairs, CHUNK):
            for c in range(tiles):
                first = natural[sweeps, c, pl.ds(2 * start, CHUNK, stride=2)]
                second = natural[sweeps, c, pl.ds(2 * start + 1, CHUNK, stride=2)]
                p0 = jnp.where(even, first, second)
                p1 = jnp.where(even, second, first)
                state[0, c, 8 + start : 8 + start + CHUNK] = p0
                state[1, c, 8 + start : 8 + start + CHUNK] = p1
                keep_edges(0, c, p0, start)
                keep_edges(1, c, p1, start)
        for w in range(sweeps):
            colour = w % 2
            other = 1 - colour
            for c in range(tiles):
                natural[w, c, :height] = draws[w, r, :, c * LANES : (c + 1) * LANES].astype(F32)
            for start in range(0, pairs, CHUNK):
                heres = [state[other, c, 8 + start : 8 + start + CHUNK] for c in range(tiles)]
                for c in range(tiles):
                    first = natural[w, c, pl.ds(2 * start, CHUNK, stride=2)]
                    second = natural[w, c, pl.ds(2 * start + 1, CHUNK, stride=2)]
                    draw = jnp.where(even, first, second) if colour == 0 else jnp.where(even, second, first)
                    keep_edges(2 + w, c, draw, start)
                    here = heres[c]
                    up = state[other, c, 7 + start : 7 + start + CHUNK]
                    down = state[other, c, 9 + start : 9 + start + CHUNK]
                    vertical = jnp.where(even, up, down) if colour == 0 else jnp.where(even, down, up)
                    left = jnp.where(lane == LANES - 1, heres[(c - 1) % tiles], here)
                    right = jnp.where(lane == 0, heres[(c + 1) % tiles], here)
                    beside = pltpu.roll(left, 1, 1) + pltpu.roll(right, LANES - 1, 1)
                    new = updated(
                        state[colour, c, 8 + start : 8 + start + CHUNK], (here + vertical) + beside, draw
                    )
                    state[colour, c, 8 + start : 8 + start + CHUNK] = new
                    if w == sweeps - 3 or w == sweeps - 1:
                        snapshot = 0 if w == sweeps - 3 else 1
                        sums[snapshot, c, start : start + CHUNK] += here + new

    together = 2 if reals % 2 == 0 else 1

    @pl.loop(0, reals // together)
    def _(step):
        for i in range(together):
            one(step * together + i, natural.at[i], state.at[i])


def strips_kernel(below, above, strips, message, corners):
    reals, tiles = below.shape[:2]
    pairs = strips.shape[2]
    lane = iota((8, LANES), 1)
    for v, source in ((0, above), (1, below)):
        sides = [jnp.zeros((8, LANES), F32) for _ in range(2)]
        for r in range(reals):
            group = lane // GROUP == r
            left = pltpu.roll(source[r, 0].astype(F32), r * GROUP + BLOCK, 1)
            right = pltpu.roll(source[r, tiles - 1].astype(F32), (r * GROUP + 12) % LANES, 1)
            sides[0] = jnp.where(group & (lane % GROUP >= BLOCK), left, sides[0])
            sides[1] = jnp.where(group, right, sides[1])
        corners[0, v] = sides[0]
        corners[1, v] = sides[1]
        message[len(NAMES) * pairs + 8 * v : len(NAMES) * pairs + 8 * v + 8] = jnp.where(
            lane % GROUP < 8, sides[0], sides[1]
        ).astype(BF16)
    lane = iota((pairs, LANES), 1)
    for index in range(len(NAMES)):
        message[index * pairs : (index + 1) * pairs] = jnp.where(
            lane % GROUP < 8, strips[index, 0], strips[index, 1]
        ).astype(BF16)


def rows_kernel(below, above, frames, inner, out, arrays):
    reals, tiles = below.shape[:2]
    sweeps = frames.shape[0] - 2
    even = even_lanes((8, LANES))
    lane = iota((8, LANES), 1)
    row = iota((8, LANES), 0)
    sides = range(2)
    for r in range(reals):
        for c in range(tiles):
            low = below[r, c].astype(F32)
            high = above[r, c].astype(F32)
            for index, name in enumerate(NAMES):
                top, bottom = halo_rows(low, high, name)
                arrays[index, r, 0, c] = jnp.where(row >= 6, top, frames[index, r, 0, c])
                arrays[index, r, 1, c] = jnp.where(row < 2, bottom, frames[index, r, 1, c])
    sums = [[[None] * tiles for _ in sides] for _ in range(2)]
    for w in range(sweeps):
        colour = w % 2
        other = 1 - colour
        for r in range(reals):
            for side in sides:
                for c in range(tiles):
                    draw = arrays[2 + w, r, side, c] if w < 3 else frames[2 + w, r, side, c]
                    here = arrays[other, r, side, c]
                    up = pltpu.roll(here, 1, 0)
                    down = pltpu.roll(here, 7, 0)
                    vertical = jnp.where(even, up, down) if colour == 0 else jnp.where(even, down, up)
                    left = arrays[other, r, side, (c - 1) % tiles]
                    right = arrays[other, r, side, (c + 1) % tiles]
                    left = pltpu.roll(jnp.where(lane == LANES - 1, left, here), 1, 1)
                    right = pltpu.roll(jnp.where(lane == 0, right, here), LANES - 1, 1)
                    new = updated(
                        arrays[colour, r, side, c], (here + vertical) + (left + right), draw
                    )
                    arrays[colour, r, side, c] = new
                    if w == sweeps - 3 or w == sweeps - 1:
                        s = 0 if w == sweeps - 3 else 1
                        both = here + new
                        before = sums[s][side][c]
                        sums[s][side][c] = both if before is None else before + both
    half = inner.shape[2] // 2
    total = jnp.zeros((2 * half, LANES), F32)
    for c in range(tiles):
        lines = []
        for s in range(2):
            cells = inner[s, c, pl.ds(0, half, stride=2)] + inner[s, c, pl.ds(1, half, stride=2)]
            top, bottom = sums[s][0][c], sums[s][1][c]
            lines.append(jnp.where(row == 0, top + pltpu.roll(top, 7, 0), cells[:8]))
            lines.append(cells[8 : half - 8])
            lines.append(jnp.where(row == 7, bottom + pltpu.roll(bottom, 1, 0), cells[half - 8 :]))
        total += selected(jnp.concatenate(lines), fold_lanes(c * (LANES // BLOCK)))
    out[0] = total[:half]
    out[1] = total[half:]


def columns_kernel(strips, corners, from_left, from_right, part, out, arrays):
    pairs = strips.shape[2]
    sweeps = strips.shape[0] - 2
    base = 16
    count = len(NAMES)
    lane = iota((pairs, LANES), 1) % GROUP
    lane8 = iota((8, LANES), 1) % GROUP
    row8 = iota((8, LANES), 0)

    def joined(side, q, own, left, right):
        if side == 0:
            return jnp.where(q < BLOCK, pltpu.roll(left, LANES - 8, 1), own)
        return jnp.where(q >= GROUP - BLOCK, pltpu.roll(right, 8, 1), own)

    zero = jnp.zeros((8, LANES), F32)
    for side in range(2):
        for index in range(count):
            rows_of = slice(index * pairs, (index + 1) * pairs)
            arrays[index, side, base : base + pairs] = joined(
                side, lane, strips[index, side], from_left[rows_of].astype(F32), from_right[rows_of].astype(F32)
            )
        halos = []
        for v in range(2):
            rows_of = slice(count * pairs + 8 * v, count * pairs + 8 * v + 8)
            halos.append(
                joined(side, lane8, corners[side, v], from_left[rows_of].astype(F32), from_right[rows_of].astype(F32))
            )
        for index, name in enumerate(NAMES):
            top, bottom = halo_rows(halos[1], halos[0], name)
            arrays[index, side, base - 8 : base] = jnp.where(row8 >= 6, top, 0.0)
            arrays[index, side, base + pairs : base + pairs + 8] = jnp.where(row8 < 2, bottom, 0.0)
            if index < 2:
                arrays[index, side, 0 : base - 8] = zero
                arrays[index, side, base + pairs + 8 : base + pairs + 16] = zero
        arrays[count, side, base : base + pairs] = strips[count, side]
        arrays[count, side, base - 8 : base] = zero
        arrays[count, side, base + pairs : base + pairs + 8] = zero
    half = pairs // 2
    for w in range(sweeps):
        colour = w % 2
        other = 1 - colour
        grow = 8 if w < sweeps - 1 else 0
        start, size = base - grow, pairs + 2 * grow
        even = even_lanes((size, LANES))
        for side in range(2):
            here = arrays[other, side, start : start + size]
            up = arrays[other, side, start - 1 : start - 1 + size]
            down = arrays[other, side, start + 1 : start + 1 + size]
            vertical = jnp.where(even, up, down) if colour == 0 else jnp.where(even, down, up)
            beside = (here + vertical) + (pltpu.roll(here, 1, 1) + pltpu.roll(here, LANES - 1, 1))
            new = updated(
                arrays[colour, side, start : start + size], beside, arrays[2 + w, side, start : start + size]
            )
            arrays[colour, side, start : start + size] = new
            if w == sweeps - 3 or w == sweeps - 1:
                s = 0 if w == sweeps - 3 else 1
                arrays[count + 1 + s, side, base : base + pairs] = (here + new)[grow : grow + pairs]
    column = iota((half, LANES), 1)
    group = column % GROUP
    for s in range(2):
        value = part[s]
        for side in range(2):
            cells = (
                arrays[count + 1 + s, side, pl.ds(base, half, stride=2)]
                + arrays[count + 1 + s, side, pl.ds(base + 1, half, stride=2)]
            )
            first = BLOCK if side == 0 else 2 * BLOCK
            own = jnp.where((group >= first) & (group < first + BLOCK), cells, 0.0)
            sums = jnp.sum(own, axis=1, keepdims=True)
            value = jnp.where(column == (0 if side == 0 else LANES - 1), sums, value)
        out[s] = value


def shifted(value, axis, by):
    count = lax.axis_size(axis)
    if count == 1:
        return value
    return lax.ppermute(value, axis, [(i, (i + by) % count) for i in range(count)])


def both_ways(to_low, to_high, axis):
    before = shifted(to_high, axis, 1)
    after = shifted(to_low, axis, -1)
    return after, before


def call(kernel, args, outs, vmem, scratch=(), flops=0, space=pltpu.VMEM):
    if space == pltpu.HBM:
        args = [pltpu.with_memory_space_constraint(arg, space) for arg in args]
    return pl.pallas_call(
        kernel,
        out_shape=tuple(pltpu.VMEM(shape, dtype) for shape, dtype in outs),
        in_specs=[pl.BlockSpec(memory_space=space) for _ in args],
        out_specs=tuple(pl.BlockSpec(memory_space=pltpu.VMEM) for _ in outs),
        scratch_shapes=list(scratch),
        compiler_params=pltpu.CompilerParams(vmem_limit_bytes=vmem * MIB),
        cost_estimate=pl.CostEstimate(flops=flops, bytes_accessed=0, transcendentals=0),
    )(*args)


ROW_STEPS = ((2, 3, 1, 0), (3, 2, 0, 1), (1, 0, 3, 2))


def integrated(occupancy, random_draws):
    reals, height, width = occupancy.shape
    sweeps = random_draws.shape[0]
    tiles, pairs, half = width // LANES, height // 2, height // BLOCK
    edge = ((reals, tiles, 8, LANES), BF16)
    low, high = call(
        edges_kernel,
        (occupancy, random_draws),
        (edge, edge),
        8,
        (
            pltpu.VMEM((2, reals, 8, width), jnp.int32),
            pltpu.VMEM((2, 3, reals, 8, width), BF16),
            pltpu.SemaphoreType.DMA((2, 2)),
        ),
        1_000_000,
        pltpu.HBM,
    )
    below, above = both_ways(low, high, "gx")
    frames, strips, inner = call(
        tile_kernel,
        (occupancy, random_draws),
        (
            ((2 + sweeps, reals, 2, tiles, 8, LANES), F32),
            ((2 + sweeps, 2, pairs, LANES), F32),
            ((2, tiles, pairs, LANES), F32),
        ),
        24,
        (
            pltpu.VMEM((2, sweeps + 1, tiles, height + 8, LANES), F32),
            pltpu.VMEM((2, 2, tiles, pairs + 16, LANES), F32),
        ),
        40_000_000,
    )
    message, corners = call(
        strips_kernel,
        (below, above, strips),
        (((len(NAMES) * pairs + 16, LANES), BF16), ((2, 2, 8, LANES), F32)),
        4,
        (),
        1_000_000,
    )
    if lax.axis_size("gy") == 2:
        from_left = from_right = shifted(message, "gy", 1)
    else:
        from_right, from_left = both_ways(message, message, "gy")
    (part,) = call(
        rows_kernel,
        (below, above, frames, inner),
        (((2, half, LANES), F32),),
        8,
        (pltpu.VMEM((len(NAMES), reals, 2, tiles, 8, LANES), F32),),
        10_000_000,
    )
    (mine,) = call(
        columns_kernel,
        (strips, corners, from_left, from_right, part),
        (((2, half, LANES), F32),),
        8,
        (pltpu.VMEM((len(NAMES) + 3, 2, pairs + 32, LANES), F32),),
        4_000_000,
    )
    count = lax.axis_size("row")
    if count == len(ROW_STEPS) + 1:
        theirs = []
        for targets in ROW_STEPS:
            theirs.append(lax.ppermute(mine, "row", list(enumerate(targets))))
        swapped = [all(t[t[i]] == i for i in range(count)) for t in ROW_STEPS].index(True)
        partner = theirs.pop(swapped)
        coarse_sums = (mine + partner) + (theirs[0] + theirs[1])
    else:
        coarse_sums = lax.psum(mine, "row")
    averages = coarse_sums * jnp.float32(1.0 / (reals * count * BLOCK * BLOCK))
    coverage = averages[1]
    projected = coverage + LEAP / 2.0 * (coverage - averages[0])
    return (coverage, projected)


def solution(mesh):
    in_specs = (P("row", "gx", "gy"), P(None, "row", "gx", "gy"))
    out_specs = (P("gx", "gy"), P("gx", "gy"))
    return jax.shard_map(integrated, mesh=mesh, in_specs=in_specs, out_specs=out_specs, check_vma=False)
```
